32 devices in a mesh: tile: 8 (over z, x), cls: 4 (over y, core).
Axes of the slice: x: 2, y: 2, z: 4, core: 2. Of those that a mesh axis runs over, the one named last changes fastest.
Arguments:
- concentration: float32 [64, 4, 16384], P('cls', None, 'tile'), may hold values from 0.05 to 2
- velocity: float32 [2, 4, 16384], P(None, None, 'tile'), may hold values from -0.3 to 0.3
- land_mask: int32 [16384], P('tile'), may hold values 0 or 1
- settling: float32 [64], P('cls'), may hold values from 0.01 to 0.3
- breakage_rate: float32 [64], replicated, may hold values from 0.02 to 0.3
- kernel_levels: int32 [64, 64], replicated, may hold values from 100 to 1000, as said below
- pair_target: int32 [64, 64], replicated, may hold values from 0 to 63, as said below
- fragment_weights: int32 [64, 64], replicated, may hold values from 1 to 16
Outputs:
- flocs: float32 [64, 4, 16384], P('cls', None, 'tile')
The draws below stay inside these ranges and needn't reach their ends.
Inputs may be any that keep to these rules, and one draw needn't show every extreme that they name: `kernel_levels`: symmetric. `pair_target`: symmetric, and entry [i, j] is at least the larger of i and j.
All inputs are finite; a program needn't handle non-finite values. No bound on the sum of `land_mask` on one device may be relied on, other than what follows from the above.
Results may differ from the reference program's by a relative error of at most 0.0001.
Values sent between devices are 32-bit elements; how exact they have to be, the bound alone decides.
A program may use at most 64 MiB of HBM per device.

```python
import math
import jax
import jax.numpy as jnp
from jax import lax

NC = 64
L = 4
CY = 512
CX = 4
COLUMNS = 16384
N_TILE = 8


def draw_kernel_levels(key, part):
    half = jax.random.randint(jax.random.fold_in(key, 11), (NC, NC), 50, 501, dtype=jnp.int32)
    return (half + half.T).astype(jnp.int32)


def draw_pair_target(key, part):
    extra = jax.random.randint(jax.random.fold_in(key, 23), (NC, NC), 0, 2, dtype=jnp.int32)
    extra = extra + extra.T
    rank = jnp.arange(NC, dtype=jnp.int32)
    larger = jnp.maximum(rank[:, None], rank[None, :])
    return jnp.minimum(larger + extra, NC - 1).astype(jnp.int32)


def plant(values, key, low, top_value):
    index_at = [jax.random.randint(jax.random.fold_in(key, axis), (), 0, length) for axis, length in enumerate(values.shape)]
    longest = values.shape.index(max(values.shape))
    next_to = index_at[:longest] + [(index_at[longest] + 1) % values.shape[longest]] + index_at[longest + 1:]
    return values.at[tuple(index_at)].set(low).at[tuple(next_to)].set(top_value)


def block_levels(rng, dims, cuts, least, largest):
    loudness = 1.0
    for position, shards_of in cuts:
        heights = jax.random.uniform(jax.random.fold_in(jax.random.fold_in(rng, 6), position), (shards_of,), jnp.float32, least / len(cuts), largest / len(cuts))
        loudness = loudness * jnp.repeat(jnp.exp(heights), dims[position] // shards_of).reshape((-1,) + (1,) * (len(dims) - 1 - position))
    return loudness


def setup_inputs(seed: int = 0) -> dict:
    key_of = jax.random.split(jax.random.key(seed), 9)
    concentration = jnp.clip(jnp.exp(math.log(2.0) - 3.6888794 * jax.random.uniform(key_of[0], (NC, L, COLUMNS), jnp.float32) ** block_levels(key_of[0], (NC, L, COLUMNS), ((0, 4), (2, 8)), -0.2, 0.2)), 0.05, 2.0)
    velocity = jnp.clip(jax.random.uniform(key_of[1], (2, L, COLUMNS), jnp.float32, -0.3, 0.3) * block_levels(key_of[1], (2, L, COLUMNS), ((2, 8),), -0.4, 0.0), -0.3, 0.3)
    land_mask = plant((jax.random.randint(key_of[2], (COLUMNS,), 0, 8) < 7).astype(jnp.int32), jax.random.fold_in(key_of[2], 1), 0, 1)
    settling = jnp.clip(jnp.exp(math.log(0.3) - 3.4011974 * jax.random.uniform(key_of[3], (NC,), jnp.float32) ** block_levels(key_of[3], (NC,), ((0, 4),), -0.2, 0.2)), 0.01, 0.3)
    breakage_rate = jnp.clip(jnp.exp(jax.random.uniform(key_of[4], (NC,), jnp.float32, math.log(0.02), math.log(0.3))), 0.02, 0.3)
    kernel_levels = draw_kernel_levels(jax.random.fold_in(key_of[8], 71), 0)
    pair_target = draw_pair_target(jax.random.fold_in(key_of[8], 71), 0)
    fragment_weights = plant(jax.random.randint(key_of[7], (NC, NC), 1, 17), jax.random.fold_in(key_of[7], 1), 1, 16).astype(jnp.int32)
    return dict(concentration=concentration, velocity=velocity, land_mask=land_mask, settling=settling, breakage_rate=breakage_rate, kernel_levels=kernel_levels, pair_target=pair_target, fragment_weights=fragment_weights)


kernel_scale = 1e-5


def to_grid(array):
    lead = array.shape[:-1]
    return array.reshape(lead + (N_TILE * CX, CY))


def from_grid(array):
    lead = array.shape[:-2]
    return array.reshape(lead + (N_TILE * CX * CY,))


def face_flux(c_low, c_high, f_low, f_high, w_low, w_high):
    speed = 0.5 * (f_low + f_high) * w_low * w_high
    return jnp.maximum(speed, 0.0) * c_low + jnp.minimum(speed, 0.0) * c_high


def reference(concentration, velocity, land_mask, settling, breakage_rate, kernel_levels, pair_target, fragment_weights):
    field = to_grid(concentration)
    speeds = to_grid(velocity)
    water = to_grid(land_mask.astype(jnp.float32))
    cpad = jnp.pad(field, ((0, 0), (0, 0), (1, 1), (1, 1)))
    spad = jnp.pad(speeds, ((0, 0), (0, 0), (1, 1), (1, 1)))
    wpad = jnp.pad(water, ((1, 1), (1, 1)))
    fx = face_flux(cpad[:, :, :-1, 1:-1], cpad[:, :, 1:, 1:-1], spad[0, :, :-1, 1:-1], spad[0, :, 1:, 1:-1], wpad[:-1, 1:-1], wpad[1:, 1:-1])
    fy = face_flux(cpad[:, :, 1:-1, :-1], cpad[:, :, 1:-1, 1:], spad[1, :, 1:-1, :-1], spad[1, :, 1:-1, 1:], wpad[1:-1, :-1], wpad[1:-1, 1:])
    moved = field - (fx[:, :, 1:] - fx[:, :, :-1]) - (fy[:, :, :, 1:] - fy[:, :, :, :-1])
    sink = settling[:, None, None, None] * field
    moved = moved - sink + jnp.pad(sink[:, :-1], ((0, 0), (1, 0), (0, 0), (0, 0)))
    current = from_grid(moved).reshape(NC, -1)

    levels = kernel_levels.astype(jnp.float32) * kernel_scale
    rank = jnp.arange(NC, dtype=jnp.int32)
    hit = pair_target[None, :, :] == rank[:, None, None]
    birth = jnp.where(hit, 0.5 * levels[None, :, :], 0.0)
    lower = jnp.where(rank[:, None] <= rank[None, :], fragment_weights.astype(jnp.float32), 0.0)
    frag = lower / jnp.sum(lower, axis=0, keepdims=True)
    by_first = jnp.transpose(birth, (1, 0, 2))
    for sub in range(2):
        def add_pair(total, item):
            table, partner = item
            made = jnp.dot(table, current, precision=lax.Precision.HIGHEST, preferred_element_type=jnp.float32)
            return total + made * partner[None, :], None
        gain, _ = lax.scan(add_pair, jnp.zeros_like(current), (by_first, current))
        loss = current * jnp.dot(levels, current, precision=lax.Precision.HIGHEST, preferred_element_type=jnp.float32)
        broken = jnp.dot(frag, breakage_rate[:, None] * current, precision=lax.Precision.HIGHEST, preferred_element_type=jnp.float32) - breakage_rate[:, None] * current
        current = current + gain - loss + broken
    return current.reshape(NC, L, N_TILE * CX * CY)
```

```python
import functools

import jax
import jax.numpy as jnp
from jax import lax
from jax.experimental import pallas as pl
from jax.experimental.pallas import tpu as pltpu
from jax.sharding import PartitionSpec as P

CY = 512
CX = 4
half_scale = 0.5e-05
STEP = 8
LANES = 128
SPLIT = 2
UNIT = CY // SPLIT


def split_pair(value, lane, total):
    high = value.astype(jnp.bfloat16).astype(jnp.float32)
    return jnp.where(lane < total, high, value - high).astype(jnp.bfloat16)


def quad_rows(total):
    return sum(STEP * (total - first) for first in range(0, total, STEP))


def build_tables(levels_ref, target_ref, weights_ref, rate_ref, quad_ref, lin_ref):
    total = levels_ref.shape[0]
    wide = 2 * total
    levels = levels_ref[...].astype(jnp.float32)
    levels = jnp.concatenate([levels, levels], 1)
    target = target_ref[...]
    target = jnp.concatenate([target, target], 1)
    row = lax.broadcasted_iota(jnp.int32, (total, wide), 0)
    lane = lax.broadcasted_iota(jnp.int32, (total, wide), 1)
    col = jnp.where(lane < total, lane, lane - total)
    twice = 2.0 * levels
    birth = jnp.where(col < row, twice, jnp.where(col == row, levels, 0.0))
    offset = 0
    for first in range(0, total, STEP):
        count = total - first
        rank = row[first:]
        for i in range(first, first + STEP):
            value = jnp.where(target[i : i + 1] == rank, birth[i : i + 1], 0.0)
            value = value - jnp.where(rank == i, twice[i : i + 1], 0.0)
            packed = split_pair(value, lane[first:], total)
            quad_ref[offset : offset + count, :wide] = packed
            quad_ref[offset : offset + count, wide:] = packed
            offset += count
    weights = weights_ref[...].astype(jnp.float32)
    weights = jnp.concatenate([weights, weights], 1)
    rate = rate_ref[...]
    rate = jnp.concatenate([rate, rate], 1)
    lower = jnp.where(row <= col, weights, 0.0)
    frag = lower / jnp.sum(lower, axis=0, keepdims=True)
    value = frag * rate - jnp.where(row == col, rate, 0.0)
    packed = split_pair(value, lane, total)
    lin_ref[:, :wide] = packed
    lin_ref[:, wide:] = packed


def react(now, quad_ref, lin_ref):
    total = now.shape[0]
    high = now.astype(jnp.bfloat16)
    low = (now - high.astype(jnp.float32)).astype(jnp.bfloat16)
    stack = jnp.concatenate([high, high, low, low], 0)
    lin = jnp.dot(lin_ref[...], stack, preferred_element_type=jnp.float32)
    gain = None
    offset = 0
    for first in range(0, total, STEP):
        count = total - first
        made = jnp.dot(
            quad_ref[offset : offset + STEP * count, :], stack, preferred_element_type=jnp.float32
        )
        part = made[:count] * now[first : first + 1]
        for r in range(1, STEP):
            part = part + made[r * count : (r + 1) * count] * now[first + r : first + r + 1]
        gain = part if gain is None else jnp.concatenate([gain[:first], gain[first:] + part], 0)
        offset += STEP * count
    return now + gain * half_scale + lin


MESH = pl.DeviceIdType.MESH


def step_kernel(
    tiles,
    peers,
    flat_hbm,
    speed_hbm,
    water_hbm,
    settling_hbm,
    rate_hbm,
    levels_hbm,
    target_hbm,
    weights_hbm,
    out_ref,
    flat_ref,
    speed_ref,
    water_ref,
    settling_ref,
    rate_ref,
    levels_ref,
    target_ref,
    weights_ref,
    quad_ref,
    lin_ref,
    field_ref,
    moved_ref,
    whole_ref,
    done_ref,
    back_ref,
    load_sem,
    halo_send,
    halo_recv,
    out_send,
    out_recv,
    back_send,
    back_recv,
):
    layers, group, columns = moved_ref.shape
    tile_lanes = columns // LANES
    own = layers // peers
    base = layers * group
    tile = lax.axis_index("tile")
    me = lax.axis_index("cls")
    has_west = tile > 0
    has_east = tile < tiles - 1

    if peers == 4:
        partners = [lax.rem(me + 2, 4), 3 - me, me + 1 - 2 * lax.rem(me, 2)]
    else:
        partners = [lax.rem(me + d, peers) for d in range(1, peers)]

    barrier = pltpu.get_barrier_semaphore()

    @pl.when(has_west)
    def _():
        pl.semaphore_signal(barrier, inc=1, device_id={"tile": tile - 1}, device_id_type=MESH)

    @pl.when(has_east)
    def _():
        pl.semaphore_signal(barrier, inc=1, device_id={"tile": tile + 1}, device_id_type=MESH)

    for p in partners:
        pl.semaphore_signal(barrier, inc=1, device_id={"cls": p}, device_id_type=MESH)

    loads = [
        pltpu.make_async_copy(source, place, load_sem.at[n])
        for n, (source, place) in enumerate(
            (
                (flat_hbm, flat_ref),
                (speed_hbm, speed_ref),
                (water_hbm, water_ref),
                (settling_hbm, settling_ref),
                (rate_hbm, rate_ref),
                (levels_hbm, levels_ref),
                (target_hbm, target_ref),
                (weights_hbm, weights_ref),
            )
        )
    ]
    for copy in loads:
        copy.start()

    def span(start, width):
        return pl.ds(pl.multiple_of(start, width), width)

    def cols(x):
        return span(x * CY, CY)

    def strip(l):
        return pl.ds(l * group, group)

    for side, there in ((0, has_west), (1, has_east)):

        @pl.when(jnp.logical_not(there))
        def _():
            field_ref[:, cols(side * (CX + 1))] = jnp.zeros((base + 2 * layers, CY), jnp.float32)

    for copy in loads[:4]:
      copy.wait()
    for l in range(layers):
        for j in range(tile_lanes):
            field_ref[strip(l), CY + j * LANES : CY + (j + 1) * LANES] = flat_ref[
                pl.ds(j * layers + l, group, stride=tile_lanes * layers), :
            ]
    inner = pl.ds(CY, columns)
    field_ref[base : base + layers, inner] = speed_ref[0]
    field_ref[base + layers : base + 2 * layers, inner] = jnp.broadcast_to(
        water_ref[...].astype(jnp.float32), (layers, columns)
    )

    before = lax.div(tile + tiles - 1, tiles)
    after = lax.div(2 * (tiles - 1) - tile, tiles)
    pl.semaphore_wait(barrier, peers - 1 + before + after)

    odd = lax.rem(tile, 2)
    near = 1 - odd
    far = odd
    first = near * (CX - 1)
    last = far * (CX - 1)

    def halo(side, way):
        return pltpu.make_async_remote_copy(
            src_ref=field_ref.at[:, cols(side * (CX - 1) + 1)],
            dst_ref=field_ref.at[:, cols((1 - side) * (CX + 1))],
            send_sem=halo_send.at[way],
            recv_sem=halo_recv.at[way],
            device_id={"tile": tile - 1 + 2 * side},
            device_id_type=MESH,
        )

    def there(side):
        return (1 - side) * tile + side * (tiles - 1 - tile) > 0

    @pl.when(there(near))
    def _():
        halo(near, 0).start()

    def forward(n, u, start, width, s):
        at = span(start, width)
        return pltpu.make_async_remote_copy(
            src_ref=moved_ref.at[partners[n] * own + s, :, at],
            dst_ref=whole_ref.at[s, span(me * group, group), at],
            send_sem=out_send,
            recv_sem=out_recv.at[u, s],
            device_id={"cls": partners[n]},
            device_id_type=MESH,
        )

    def backward(n, q, start, width, s):
        at = span(start, width)
        return pltpu.make_async_remote_copy(
            src_ref=done_ref.at[s, span(partners[n] * group, group), at],
            dst_ref=back_ref.at[me * own + s, :, at],
            send_sem=back_send,
            recv_sem=back_recv.at[q],
            device_id={"cls": partners[n]},
            device_id_type=MESH,
        )

    def await_all(ref, sem):
        pltpu.make_async_copy(ref, ref, sem).wait()

    square = (group, group)
    diagonal = lax.broadcasted_iota(jnp.int32, square, 0) == lax.broadcasted_iota(
        jnp.int32, square, 1
    )
    settle = jnp.sum(jnp.where(diagonal, settling_ref[...], 0.0), axis=1, keepdims=True)
    settle = jnp.broadcast_to(settle, (group, CY))

    def transport(u, x, pieces):
        at = cols(x + 1)
        u_of = pl.ds(base, layers)
        w_of = pl.ds(base + layers, layers)
        speed, water = field_ref[u_of, at], field_ref[w_of, at]
        face_low = 0.5 * (field_ref[u_of, cols(x)] + speed) * (field_ref[w_of, cols(x)] * water)
        face_high = (
            0.5 * (speed + field_ref[u_of, cols(x + 2)]) * (water * field_ref[w_of, cols(x + 2)])
        )
        v = speed_ref[1, :, cols(x)]
        lane = lax.broadcasted_iota(jnp.int32, v.shape, 1)
        side_high = 0.5 * (v + pltpu.roll(v, CY - 1, 1)) * (water * pltpu.roll(water, CY - 1, 1))
        side_high = jnp.where(lane == CY - 1, 0.0, side_high)
        side_low = pltpu.roll(side_high, 1, 1)
        up = jnp.maximum
        down = jnp.minimum
        centre = (
            1.0 - up(face_high, 0.0) + down(face_low, 0.0) - up(side_high, 0.0) + down(side_low, 0.0)
        )
        west = up(face_low, 0.0)
        east = -down(face_high, 0.0)
        south = up(side_low, 0.0)
        north = -down(side_high, 0.0)
        for l in range(layers):
            c = field_ref[strip(l), at]
            moved = (
                (centre[l : l + 1] - settle) * c
                + west[l : l + 1] * field_ref[strip(l), cols(x)]
                + east[l : l + 1] * field_ref[strip(l), cols(x + 2)]
                + south[l : l + 1] * pltpu.roll(c, 1, 1)
                + north[l : l + 1] * pltpu.roll(c, CY - 1, 1)
            )
            if l > 0:
                moved = moved + settle * field_ref[strip(l - 1), at]
            moved_ref[l, :, cols(x)] = moved
        width = CY // pieces
        for h in range(pieces):
            for s in range(own):
                for n in range(peers - 1):
                    forward(n, u + h, x * CY + h * width, width, s).start()
        for s in range(own):
            whole_ref[s, span(me * group, group), cols(x)] = moved_ref[me * own + s, :, cols(x)]

    for x in range(1, CX - 1):
        transport(x - 1, x, 1)

    for copy in loads[4:]:
      copy.wait()
    build_tables(levels_ref, target_ref, weights_ref, rate_ref, quad_ref, lin_ref)

    @pl.when(there(near))
    def _():
        halo(near, 0).wait_send()

    @pl.when(there(far))
    def _():
        halo(far, 1).start()

    def edge(side, way, u, x, pieces):
        @pl.when(there(side))
        def _():
            halo(side, way).wait_recv()

        transport(u, x, pieces)

    def unit(u, q, start, width):
        at = span(start, width)
        for s in range(own):
            await_all(whole_ref.at[s, pl.ds(0, (peers - 1) * group), at], out_recv.at[u, s])
            now = react(whole_ref[s, :, at], quad_ref, lin_ref)
            done_ref[s, :, at] = react(now, quad_ref, lin_ref)
            for n in range(peers - 1):
                backward(n, q, start, width, s).start()
            back_ref[me * own + s, :, at] = done_ref[s, span(me * group, group), at]

    rows = CX - 1

    def full(q, carry):
        @pl.when(q == NEAR_AT)
        def _():
            edge(near, 0, CX - 2, first, 1)

        @pl.when(q == FAR_AT)
        def _():
            edge(far, 1, CX - 1, last, SPLIT)

        a = lax.div(q, CX - 2)
        x = (1 - a) * (q + 1) + a * first
        unit(q, q, x * CY, CY)
        return carry

    lax.fori_loop(0, rows, full, 0)

    def piece(h, carry):
        unit(rows + h, rows, last * CY + h * UNIT, UNIT)
        return carry

    lax.fori_loop(0, SPLIT, piece, 0)

    @pl.when(there(far))
    def _():
        halo(far, 1).wait_send()

    def finish(q, x):
        await_all(back_ref.at[pl.ds(0, (peers - 1) * own), :, cols(x)], back_recv.at[q])
        for l in range(layers):
            for j in range(CY // LANES):
                at = (x * (CY // LANES) + j) * layers + l
                out_ref[pl.ds(at, group, stride=tile_lanes * layers), :] = back_ref[
                    l, :, span(x * CY + j * LANES, LANES)
                ]

    await_all(moved_ref.at[pl.ds(0, (peers - 1) * own)], out_send)
    for q in range(CX):
        finish(q, (*range(1, CX - 1), first, last)[q])
    await_all(done_ref.at[:, pl.ds(0, (peers - 1) * group), :], back_send)


NEAR_AT = 1
FAR_AT = 2


def body(
    tiles,
    peers,
    concentration,
    velocity,
    land_mask,
    settling,
    breakage_rate,
    kernel_levels,
    pair_target,
    fragment_weights,
):
    group, layers, columns = concentration.shape
    total = kernel_levels.shape[0]
    own = layers // peers
    flat = concentration.reshape(group, layers, columns // LANES, LANES)
    flat = jnp.transpose(flat, (0, 2, 1, 3)).reshape(-1, LANES)
    operands = (
        flat,
        velocity,
        land_mask.reshape(1, columns),
        settling.reshape(1, group),
        breakage_rate.reshape(1, total),
        kernel_levels,
        pair_target,
        fragment_weights,
    )
    dma = pltpu.SemaphoreType.DMA
    done = pl.pallas_call(
        functools.partial(step_kernel, tiles, peers),
        out_shape=pltpu.VMEM((group * layers * columns // LANES, LANES), jnp.float32),
        in_specs=[pl.BlockSpec(memory_space=pl.ANY)] * len(operands),
        out_specs=pl.BlockSpec(memory_space=pltpu.VMEM),
        scratch_shapes=[
            pltpu.VMEM(flat.shape, jnp.float32),
            *[pltpu.VMEM(x.shape, x.dtype) for x in operands[1:]],
            pltpu.VMEM((quad_rows(total), 4 * total), jnp.bfloat16),
            pltpu.VMEM((total, 4 * total), jnp.bfloat16),
            pltpu.VMEM((layers * (group + 2), columns + 2 * CY), jnp.float32),
            pltpu.VMEM((layers, group, columns), jnp.float32),
            pltpu.VMEM((own, total, columns), jnp.float32),
            pltpu.VMEM((own, total, columns), jnp.float32),
            pltpu.VMEM((layers, group, columns), jnp.float32),
            dma((len(operands),)),
            dma((2,)),
            dma((2,)),
            dma,
            dma((CX - 1 + SPLIT, own)),
            dma,
            dma((CX,)),
        ],
        compiler_params=pltpu.CompilerParams(collective_id=0, has_side_effects=True),
    )(*operands)
    done = done.reshape(group, columns // LANES, layers, LANES)
    return jnp.transpose(done, (0, 2, 1, 3)).reshape(group, layers, columns)


def solution(mesh):
    return jax.shard_map(
        functools.partial(body, mesh.shape["tile"], mesh.shape["cls"]),
        mesh=mesh,
        in_specs=(
            P("cls", None, "tile"),
            P(None, None, "tile"),
            P("tile"),
            P("cls"),
            P(),
            P(),
            P(),
            P(),
        ),
        out_specs=P("cls", None, "tile"),
        check_vma=False,
    )
```

```python
import functools

import jax
import jax.numpy as jnp
from jax import lax
from jax.experimental import pallas as pl
from jax.experimental.pallas import tpu as pltpu
from jax.sharding import PartitionSpec as P

CY = 512
CX = 4
half_scale = 0.5e-05
STEP = 8
EDGE = 16
LANES = 128
SPLIT = 2
UNIT = CY // SPLIT


def split_pair(value, lane, total):
    high = value.astype(jnp.bfloat16).astype(jnp.float32)
    return jnp.where(lane < total, high, value - high).astype(jnp.bfloat16)


def halves(value):
    high = value.astype(jnp.bfloat16)
    return high, (value - high.astype(jnp.float32)).astype(jnp.bfloat16)


def pair_span(i):
    return STEP * (i // STEP + 1)


def quad_rows(total):
    return sum(STEP * (total - first) for first in range(EDGE, total, STEP)) + EDGE


def pair_rows():
    return sum(pair_span(i) for i in range(EDGE))


def build_tables(levels_ref, target_ref, weights_ref, rate_ref, quad_ref, pair_ref):
    total = levels_ref.shape[0]
    wide = 2 * total
    narrow = levels_ref[...].astype(jnp.float32)
    levels = jnp.concatenate([narrow, narrow], 1)
    target = target_ref[...]
    target = jnp.concatenate([target, target], 1)
    row = lax.broadcasted_iota(jnp.int32, (total, wide), 0)
    lane = lax.broadcasted_iota(jnp.int32, (total, wide), 1)
    col = jnp.where(lane < total, lane, lane - total)
    twice = 2.0 * levels
    birth = jnp.where(col < row, twice, jnp.where(col == row, levels, 0.0))

    def put(offset, value, lane):
        count = value.shape[0]
        packed = split_pair(value, lane, total)
        quad_ref[offset : offset + count, :wide] = packed
        quad_ref[offset : offset + count, wide:] = packed
        return offset + count

    offset = 0
    for first in range(EDGE, total, STEP):
        rank = row[first:]
        for i in range(first, first + STEP):
            value = jnp.where(target[i : i + 1] == rank, birth[i : i + 1], 0.0)
            value = value - jnp.where(rank == i, twice[i : i + 1], 0.0)
            offset = put(offset, value, lane[first:])
    put(offset, jnp.where(col[:EDGE] >= EDGE, twice[:EDGE], 0.0), lane[:EDGE])

    count = pair_rows()

    def flat(make):
        return jnp.concatenate([make(i, pair_span(i)) for i in range(EDGE)], 1)

    rank = lax.broadcasted_iota(jnp.int32, (total, count), 0)
    one = flat(lambda i, width: jnp.full((1, width), i, jnp.int32))
    other = flat(lambda i, width: lax.broadcasted_iota(jnp.int32, (1, width), 1))
    goal = flat(lambda i, width: target_ref[i : i + 1, :width])
    level = flat(lambda i, width: 2.0 * levels_ref[i : i + 1, :width].astype(jnp.float32))
    level = jnp.where(other <= one, level, 0.0)
    same = other == one
    value = jnp.where(rank == goal, jnp.where(same, 0.5 * level, level), 0.0)
    value = value - jnp.where(rank == one, level, 0.0)
    value = value - jnp.where(rank == other, jnp.where(same, 0.0, level), 0.0)
    square = (total, total)
    row = lax.broadcasted_iota(jnp.int32, square, 0)
    col = lax.broadcasted_iota(jnp.int32, square, 1)
    lower = jnp.where(row <= col, weights_ref[...].astype(jnp.float32), 0.0)
    frag = lower / jnp.sum(lower, axis=0, keepdims=True)
    rate = rate_ref[...]
    linear = (frag * rate - jnp.where(row == col, rate, 0.0)) * (1.0 / half_scale)
    high, low = halves(jnp.concatenate([value, linear], 1))
    pair_ref[:total] = high
    pair_ref[total:] = low


def react(now, quad_ref, pair_ref):
    total = now.shape[0]
    high, low = halves(now)
    stack = jnp.concatenate([high, high, low, low], 0)
    ahead = [now[: pair_span(i)] * now[i : i + 1] for i in range(EDGE)]
    high, low = halves(jnp.concatenate([*ahead, now], 0))

    def dot(table, value):
        return jnp.dot(table, value, preferred_element_type=jnp.float32)

    def made_of(offset, count):
        return dot(quad_ref[offset : offset + count, :], stack)

    gain = None
    offset = 0
    for first in range(EDGE, total, STEP):
        count = total - first
        made = made_of(offset, STEP * count)
        part = made[:count] * now[first : first + 1]
        for r in range(1, STEP):
            part = part + made[r * count : (r + 1) * count] * now[first + r : first + r + 1]
        skip = first - EDGE
        gain = part if gain is None else jnp.concatenate([gain[:skip], gain[skip:] + part], 0)
        offset += STEP * count
    loss = made_of(offset, EDGE) * now[:EDGE]
    both = dot(pair_ref[...], high)
    rest = both[:total] + both[total:] + dot(pair_ref[:total], low)
    return now + (rest + jnp.concatenate([-loss, gain], 0)) * half_scale


MESH = pl.DeviceIdType.MESH
LAND = 4.0


def step_kernel(
    tiles,
    peers,
    flat_hbm,
    speed_hbm,
    water_hbm,
    settling_hbm,
    rate_hbm,
    levels_hbm,
    target_hbm,
    weights_hbm,
    out_ref,
    flat_ref,
    speed_ref,
    water_ref,
    settling_ref,
    rate_ref,
    levels_ref,
    target_ref,
    weights_ref,
    quad_ref,
    pair_ref,
    field_ref,
    drift_ref,
    outer_ref,
    halo_ref,
    moved_ref,
    whole_ref,
    done_ref,
    back_ref,
    load_sem,
    drift_send,
    drift_recv,
    halo_send,
    halo_recv,
    out_send,
    out_recv,
    back_send,
    back_recv,
):
    layers, group, columns = moved_ref.shape
    tile_lanes = columns // LANES
    own = layers // peers
    tile = lax.axis_index("tile")
    me = lax.axis_index("cls")
    has_west = tile > 0
    has_east = tile < tiles - 1

    if peers == 4:
        partners = [lax.rem(me + 2, 4), 3 - me, me + 1 - 2 * lax.rem(me, 2)]
    else:
        partners = [lax.rem(me + d, peers) for d in range(1, peers)]

    barrier = pltpu.get_barrier_semaphore()

    @pl.when(has_west)
    def _():
        pl.semaphore_signal(barrier, inc=1, device_id={"tile": tile - 1}, device_id_type=MESH)

    @pl.when(has_east)
    def _():
        pl.semaphore_signal(barrier, inc=1, device_id={"tile": tile + 1}, device_id_type=MESH)

    for p in partners:
        pl.semaphore_signal(barrier, inc=1, device_id={"cls": p}, device_id_type=MESH)

    loads = [
        pltpu.make_async_copy(source, place, load_sem.at[n])
        for n, (source, place) in enumerate(
            (
                (flat_hbm, flat_ref),
                (speed_hbm, speed_ref),
                (water_hbm, water_ref),
                (settling_hbm, settling_ref),
                (rate_hbm, rate_ref),
                (levels_hbm, levels_ref),
                (target_hbm, target_ref),
                (weights_hbm, weights_ref),
            )
        )
    ]
    for copy in loads:
        copy.start()

    def span(start, width):
        return pl.ds(pl.multiple_of(start, width), width)

    def cols(x):
        return span(x * CY, CY)

    def strip(l):
        return pl.ds(l * group, group)

    for side, exists in ((0, has_west), (1, has_east)):

        @pl.when(jnp.logical_not(exists))
        def _():
            drift_ref[:, cols(side * (CX + 1))] = jnp.full((layers, CY), LAND, jnp.float32)

    for copy in loads[:4]:
      copy.wait()
    drift_ref[:, pl.ds(CY, columns)] = jnp.where(
        jnp.broadcast_to(water_ref[...], (layers, columns)) == 1, speed_ref[0], LAND
    )
    for l in range(layers):
        for j in range(tile_lanes):
            field_ref[strip(l), j * LANES : (j + 1) * LANES] = flat_ref[
                pl.ds(j * layers + l, group, stride=tile_lanes * layers), :
            ]

    before = lax.div(tile + tiles - 1, tiles)
    after = lax.div(2 * (tiles - 1) - tile, tiles)
    pl.semaphore_wait(barrier, peers - 1 + before + after)

    far_side = lax.rem(tile, 2)
    sides = (far_side, 1 - far_side)
    edges = [side * (CX - 1) for side in sides]

    def there(way):
        side = sides[way]
        return (1 - side) * tile + side * (tiles - 1 - tile) > 0

    def beyond(way):
        return {"tile": tile - 1 + 2 * sides[way]}

    def drift(way):
        side = sides[way]
        return pltpu.make_async_remote_copy(
            src_ref=drift_ref.at[:, cols(edges[way] + 1)],
            dst_ref=drift_ref.at[:, cols((1 - side) * (CX + 1))],
            send_sem=drift_send.at[way],
            recv_sem=drift_recv.at[way],
            device_id=beyond(way),
            device_id_type=MESH,
        )

    def halo(way, h):
        return pltpu.make_async_remote_copy(
            src_ref=field_ref.at[:, span(edges[way] * CY + h * UNIT, UNIT)],
            dst_ref=halo_ref.at[way, :, pl.ds(h * UNIT, UNIT)],
            send_sem=halo_send.at[way],
            recv_sem=halo_recv.at[way, h],
            device_id=beyond(way),
            device_id_type=MESH,
        )

    for way in range(2):

        @pl.when(there(way))
        def _():
            drift(way).start()

    for way in HALO_ORDER:

        @pl.when(there(way))
        def _():
            for h in range(SPLIT):
                halo(way, h).start()

    def await_all(ref, sem):
        pltpu.make_async_copy(ref, ref, sem).wait()

    def forward(n, u, start, width, s):
        at = span(start, width)
        return pltpu.make_async_remote_copy(
            src_ref=moved_ref.at[partners[n] * own + s, :, at],
            dst_ref=whole_ref.at[s, span(me * group, group), at],
            send_sem=out_send,
            recv_sem=out_recv.at[u, s],
            device_id={"cls": partners[n]},
            device_id_type=MESH,
        )

    def send(u, start, width):
        for s in range(own):
            for n in range(peers - 1):
                forward(n, u, start, width, s).start()
        at = span(start, width)
        for s in range(own):
            whole_ref[s, span(me * group, group), at] = moved_ref[me * own + s, :, at]

    def backward(n, u, start, width, s):
        at = span(start, width)
        return pltpu.make_async_remote_copy(
            src_ref=done_ref.at[s, span(partners[n] * group, group), at],
            dst_ref=back_ref.at[me * own + s, :, at],
            send_sem=back_send,
            recv_sem=back_recv.at[u],
            device_id={"cls": partners[n]},
            device_id_type=MESH,
        )

    square = (group, group)
    diagonal = lax.broadcasted_iota(jnp.int32, square, 0) == lax.broadcasted_iota(
        jnp.int32, square, 1
    )
    settle = jnp.sum(jnp.where(diagonal, settling_ref[...], 0.0), axis=1, keepdims=True)
    settle = jnp.broadcast_to(settle, (group, CY))

    def transport(x, way=None):
        def row(at):
            value = drift_ref[:, cols(at)]
            return value, jnp.where(value < 0.5 * LAND, 1.0, 0.0)

        speed, water = row(x + 1)
        speed_low, water_low = row(x)
        speed_high, water_high = row(x + 2)
        face_low = 0.5 * (speed_low + speed) * (water_low * water)
        face_high = 0.5 * (speed + speed_high) * (water * water_high)
        v = speed_ref[1, :, cols(x)]
        lane = lax.broadcasted_iota(jnp.int32, v.shape, 1)
        side_high = 0.5 * (v + pltpu.roll(v, CY - 1, 1)) * (water * pltpu.roll(water, CY - 1, 1))
        side_high = jnp.where(lane == CY - 1, 0.0, side_high)
        side_low = pltpu.roll(side_high, 1, 1)
        up = jnp.maximum
        down = jnp.minimum
        centre = (
            1.0 - up(face_high, 0.0) + down(face_low, 0.0) - up(side_high, 0.0) + down(side_low, 0.0)
        )
        west = up(face_low, 0.0)
        east = -down(face_high, 0.0)
        south = up(side_low, 0.0)
        north = -down(side_high, 0.0)
        if way is None:
            inner = ((west, x - 1), (east, x + 1))
        else:
            eastern = sides[way] == 1
            outer_ref[way] = jnp.where(eastern, east, west)
            inner = ((jnp.where(eastern, west, east), x + 1 - 2 * sides[way]),)
        for l in range(layers):
            c = field_ref[strip(l), cols(x)]
            moved = (
                (centre[l : l + 1] - settle) * c
                + south[l : l + 1] * pltpu.roll(c, 1, 1)
                + north[l : l + 1] * pltpu.roll(c, CY - 1, 1)
            )
            for factor, at in inner:
                moved = moved + factor[l : l + 1] * field_ref[strip(l), cols(at)]
            if l > 0:
                moved = moved + settle * field_ref[strip(l - 1), cols(x)]
            moved_ref[l, :, cols(x)] = moved

    rows = CX - 2

    def prepare(way):
        @pl.when(there(way))
        def _():
            with jax.named_scope(f'driftwait{way}'):
                drift(way).wait_recv()

        transport(edges[way], way)

    def close(way):
        for h in range(SPLIT):
            start = edges[way] * CY + h * UNIT

            @pl.when(there(way))
            def _():
                with jax.named_scope(f'halowait{way}'):
                    halo(way, h).wait_recv()
                at = pl.ds(h * UNIT, UNIT)
                for l in range(layers):
                    moved_ref[l, :, span(start, UNIT)] += (
                        outer_ref[way, l : l + 1, at] * halo_ref[way, strip(l), at]
                    )

            send((rows + way) * SPLIT + h, start, UNIT)

    for x in range(1, CX - 1):
        transport(x)
        for h in range(SPLIT):
            send((x - 1) * SPLIT + h, x * CY + h * UNIT, UNIT)

    for copy in loads[4:]:
      copy.wait()
    build_tables(levels_ref, target_ref, weights_ref, rate_ref, quad_ref, pair_ref)

    @pl.when(jnp.logical_not(there(0)))
    def _():
        prepare(0)
        close(0)

    def slot(k):
        return lax.div(k, SPLIT) + lax.div(k, CX * SPLIT - 1) * (SPLIT - 1)

    def unit(u, start, width):
        at = span(start, width)
        for s in range(own):
            await_all(whole_ref.at[s, pl.ds(0, (peers - 1) * group), at], out_recv.at[u, s])
            now = react(whole_ref[s, :, at], quad_ref, pair_ref)
            done_ref[s, :, at] = react(now, quad_ref, pair_ref)
            for n in range(peers - 1):
                backward(n, slot(u), start, width, s).start()
            back_ref[me * own + s, :, at] = done_ref[s, span(me * group, group), at]

    def step(k, carry):
        for at, way, act in ((PREP_A, 0, prepare), (CLOSE_A, 0, close)):

            @pl.when(jnp.logical_and(k == at, there(0)))
            def _():
                act(way)

        for at, way, act in ((PREP_B, 1, prepare), (CLOSE_B, 1, close)):

            @pl.when(k == at)
            def _():
                act(way)

        q = lax.div(k, SPLIT)
        outer = lax.div(q, rows)
        b = lax.rem(q, rows)
        x = (1 - outer) * (q + 1) + outer * ((1 - b) * edges[0] + b * edges[1])
        unit(k, x * CY + lax.rem(k, SPLIT) * UNIT, UNIT)
        return carry

    lax.fori_loop(0, CX * SPLIT, step, 0)

    for way in range(2):

        @pl.when(there(way))
        def _():
            drift(way).wait_send()
            await_all(halo_ref.at[way], halo_send.at[way])

    def finish(u, start, width):
        await_all(
            back_ref.at[pl.ds(0, (peers - 1) * own), :, span(start, width)], back_recv.at[u]
        )
        for l in range(layers):
            for j in range(width // LANES):
                at = (lax.div(start, LANES) + j) * layers + l
                out_ref[pl.ds(at, group, stride=tile_lanes * layers), :] = back_ref[
                    l, :, span(start + j * LANES, LANES)
                ]

    await_all(moved_ref.at[pl.ds(0, (peers - 1) * own)], out_send)
    for q in range(rows):
        finish(q, (q + 1) * CY, CY)
    finish(rows, edges[0] * CY, CY)
    for h in range(SPLIT):
        finish(rows + 1 + h, edges[1] * CY + h * UNIT, UNIT)
    await_all(done_ref.at[:, pl.ds(0, (peers - 1) * group), :], back_send)


PREP_A = 2
CLOSE_A = 2
PREP_B = 3
CLOSE_B = 3
HALO_ORDER = (0, 1)


def body(
    tiles,
    peers,
    concentration,
    velocity,
    land_mask,
    settling,
    breakage_rate,
    kernel_levels,
    pair_target,
    fragment_weights,
):
    group, layers, columns = concentration.shape
    total = kernel_levels.shape[0]
    own = layers // peers
    flat = concentration.reshape(group, layers, columns // LANES, LANES)
    flat = jnp.transpose(flat, (0, 2, 1, 3)).reshape(-1, LANES)
    operands = (
        flat,
        velocity,
        land_mask.reshape(1, columns),
        settling.reshape(1, group),
        breakage_rate.reshape(1, total),
        kernel_levels,
        pair_target,
        fragment_weights,
    )
    dma = pltpu.SemaphoreType.DMA
    done = pl.pallas_call(
        functools.partial(step_kernel, tiles, peers),
        out_shape=pltpu.VMEM((group * layers * columns // LANES, LANES), jnp.float32),
        in_specs=[pl.BlockSpec(memory_space=pl.ANY)] * len(operands),
        out_specs=pl.BlockSpec(memory_space=pltpu.VMEM),
        scratch_shapes=[
            pltpu.VMEM(flat.shape, jnp.float32),
            *[pltpu.VMEM(x.shape, x.dtype) for x in operands[1:]],
            pltpu.VMEM((quad_rows(total), 4 * total), jnp.bfloat16),
            pltpu.VMEM((2 * total, pair_rows() + total), jnp.bfloat16),
            pltpu.VMEM((layers * group, columns), jnp.float32),
            pltpu.VMEM((layers, columns + 2 * CY), jnp.float32),
            pltpu.VMEM((2, layers, CY), jnp.float32),
            pltpu.VMEM((2, layers * group, CY), jnp.float32),
            pltpu.VMEM((layers, group, columns), jnp.float32),
            pltpu.VMEM((own, total, columns), jnp.float32),
            pltpu.VMEM((own, total, columns), jnp.float32),
            pltpu.VMEM((layers, group, columns), jnp.float32),
            dma((len(operands),)),
            dma((2,)),
            dma((2,)),
            dma((2,)),
            dma((2, SPLIT)),
            dma,
            dma((CX * SPLIT, own)),
            dma,
            dma((CX - 1 + SPLIT,)),
        ],
        compiler_params=pltpu.CompilerParams(collective_id=0, has_side_effects=True),
    )(*operands)
    done = done.reshape(group, columns // LANES, layers, LANES)
    return jnp.transpose(done, (0, 2, 1, 3)).reshape(group, layers, columns)


def solution(mesh):
    return jax.shard_map(
        functools.partial(body, mesh.shape["tile"], mesh.shape["cls"]),
        mesh=mesh,
        in_specs=(
            P("cls", None, "tile"),
            P(None, None, "tile"),
            P("tile"),
            P("cls"),
            P(),
            P(),
            P(),
            P(),
        ),
        out_specs=P("cls", None, "tile"),
        check_vma=False,
    )
```

```python
import functools

import jax
import jax.numpy as jnp
from jax import lax
from jax.experimental import pallas as pl
from jax.experimental.pallas import tpu as pltpu
from jax.sharding import PartitionSpec as P

CY = 512
CX = 4
half_scale = 0.5e-05
STEP = 8
EDGE = 16
LARGEST = 448
LANES = 128
SPLIT = 2
UNIT = CY // SPLIT
UNITS = CX - 2 + 2 * SPLIT


def split_pair(value, lane, total):
    high = value.astype(jnp.bfloat16).astype(jnp.float32)
    return jnp.where(lane < total, high, value - high).astype(jnp.bfloat16)


def halves(value):
    high = value.astype(jnp.bfloat16)
    return high, (value - high.astype(jnp.float32)).astype(jnp.bfloat16)


def pair_span(i):
    return STEP * (i // STEP + 1)


def quad_rows(total):
    return sum(STEP * (total - first) for first in range(EDGE, total, STEP)) + EDGE


def pair_rows():
    return sum(pair_span(i) for i in range(EDGE))


def build_tables(levels_ref, target_ref, weights_ref, rate_ref, quad_ref, pair_ref):
    total = levels_ref.shape[0]
    wide = 2 * total
    narrow = levels_ref[...].astype(jnp.float32)
    levels = jnp.concatenate([narrow, narrow], 1)
    target = target_ref[...]
    target = jnp.concatenate([target, target], 1)
    row = lax.broadcasted_iota(jnp.int32, (total, wide), 0)
    lane = lax.broadcasted_iota(jnp.int32, (total, wide), 1)
    col = jnp.where(lane < total, lane, lane - total)
    twice = 2.0 * levels
    birth = jnp.where(col < row, twice, jnp.where(col == row, levels, 0.0))

    def put(offset, value, lane):
        count = value.shape[0]
        packed = split_pair(value, lane, total)
        quad_ref[offset : offset + count, :wide] = packed
        quad_ref[offset : offset + count, wide:] = packed
        return offset + count

    offset = 0
    for first in range(EDGE, total, STEP):
        rank = row[first:]
        for i in range(first, first + STEP):
            value = jnp.where(target[i : i + 1] == rank, birth[i : i + 1], 0.0)
            value = value - jnp.where(rank == i, twice[i : i + 1], 0.0)
            offset = put(offset, value, lane[first:])
    put(offset, jnp.where(col[:EDGE] >= EDGE, twice[:EDGE], 0.0), lane[:EDGE])

    count = pair_rows()

    def flat(make):
        return jnp.concatenate([make(i, pair_span(i)) for i in range(EDGE)], 1)

    rank = lax.broadcasted_iota(jnp.int32, (total, count), 0)
    one = flat(lambda i, width: jnp.full((1, width), i, jnp.int32))
    other = flat(lambda i, width: lax.broadcasted_iota(jnp.int32, (1, width), 1))
    goal = flat(lambda i, width: target_ref[i : i + 1, :width])
    level = flat(lambda i, width: 2.0 * levels_ref[i : i + 1, :width].astype(jnp.float32))
    level = jnp.where(other <= one, level, 0.0)
    same = other == one
    value = jnp.where(rank == goal, jnp.where(same, 0.5 * level, level), 0.0)
    value = value - jnp.where(rank == one, level, 0.0)
    value = value - jnp.where(rank == other, jnp.where(same, 0.0, level), 0.0)
    square = (total, total)
    row = lax.broadcasted_iota(jnp.int32, square, 0)
    col = lax.broadcasted_iota(jnp.int32, square, 1)
    lower = jnp.where(row <= col, weights_ref[...].astype(jnp.float32), 0.0)
    frag = lower / jnp.sum(lower, axis=0, keepdims=True)
    rate = rate_ref[...]
    linear = (frag * rate - jnp.where(row == col, rate, 0.0)) * (1.0 / half_scale)
    high, low = halves(jnp.concatenate([value, linear], 1))
    pair_ref[:total] = high
    pair_ref[total:] = low


def react(now, quad_ref, pair_ref):
    total = now.shape[0]
    high, low = halves(now)
    stack = jnp.concatenate([high, high, low, low], 0)
    ahead = [now[: pair_span(i)] * now[i : i + 1] for i in range(EDGE)]
    high, low = halves(jnp.concatenate([*ahead, now], 0))

    def dot(table, value):
        return jnp.dot(table, value, preferred_element_type=jnp.float32)

    spans = [(first, STEP * (total - first)) for first in range(EDGE, total, STEP)] + [(None, EDGE)]
    made = {}
    offset = 0
    while spans:
        taken = [spans.pop(0)]
        while spans and sum(count for _, count in taken) + spans[0][1] <= LARGEST:
            taken.append(spans.pop(0))
        count = sum(count for _, count in taken)
        product = dot(quad_ref[offset : offset + count, :], stack)
        offset += count
        start = 0
        for first, count in taken:
            made[first] = product[start : start + count]
            start += count

    gain = None
    for first in range(EDGE, total, STEP):
        count = total - first
        part = made[first][:count] * now[first : first + 1]
        for r in range(1, STEP):
            part = part + made[first][r * count : (r + 1) * count] * now[first + r : first + r + 1]
        skip = first - EDGE
        gain = part if gain is None else jnp.concatenate([gain[:skip], gain[skip:] + part], 0)
    loss = made[None] * now[:EDGE]
    both = dot(pair_ref[...], high)
    rest = both[:total] + both[total:] + dot(pair_ref[:total], low)
    return now + (rest + jnp.concatenate([-loss, gain], 0)) * half_scale


MESH = pl.DeviceIdType.MESH
LAND = 4.0


def step_kernel(
    tiles,
    peers,
    flat_hbm,
    speed_hbm,
    water_hbm,
    settling_hbm,
    rate_hbm,
    levels_hbm,
    target_hbm,
    weights_hbm,
    out_ref,
    flat_ref,
    speed_ref,
    water_ref,
    settling_ref,
    rate_ref,
    table_ref,
    quad_ref,
    pair_ref,
    field_ref,
    drift_ref,
    outer_ref,
    halo_ref,
    moved_ref,
    whole_ref,
    done_ref,
    back_ref,
    load_sem,
    drift_recv,
    halo_recv,
    out_send,
    out_recv,
    back_recv,
):
    layers, group, columns = moved_ref.shape
    tile_lanes = columns // LANES
    block = CY // LANES * layers
    own = layers // peers
    tile = lax.axis_index("tile")
    me = lax.axis_index("cls")
    has_west = tile > 0
    has_east = tile < tiles - 1

    if peers == 4:
        partners = [lax.rem(me + 2, 4), 3 - me, me + 1 - 2 * lax.rem(me, 2)]
    else:
        partners = [lax.rem(me + d, peers) for d in range(1, peers)]

    barrier = pltpu.get_barrier_semaphore()

    @pl.when(has_west)
    def _():
        pl.semaphore_signal(barrier, inc=1, device_id={"tile": tile - 1}, device_id_type=MESH)

    @pl.when(has_east)
    def _():
        pl.semaphore_signal(barrier, inc=1, device_id={"tile": tile + 1}, device_id_type=MESH)

    for p in partners:
        pl.semaphore_signal(barrier, inc=1, device_id={"cls": p}, device_id_type=MESH)

    loads = [
        pltpu.make_async_copy(source, place, load_sem.at[n])
        for n, (source, place) in enumerate(
            (
                (flat_hbm, flat_ref),
                (speed_hbm, speed_ref),
                (water_hbm, water_ref),
                (settling_hbm, settling_ref),
                (rate_hbm, rate_ref),
            )
        )
    ]
    for copy in loads:
        copy.start()
    for n, source in enumerate((levels_hbm, target_hbm, weights_hbm)):
        pltpu.make_async_copy(source, table_ref.at[n], load_sem.at[len(loads)]).start()

    def span(start, width):
        return pl.ds(pl.multiple_of(start, width), width)

    def cols(x):
        return span(x * CY, CY)

    def strip(l):
        return pl.ds(l * group, group)

    for side, exists in ((0, has_west), (1, has_east)):

        @pl.when(jnp.logical_not(exists))
        def _():
            drift_ref[:, cols(side * (CX + 1))] = jnp.full((layers, CY), LAND, jnp.float32)

    for copy in loads[:4]:
        copy.wait()
    drift_ref[:, pl.ds(CY, columns)] = jnp.where(
        jnp.broadcast_to(water_ref[...], (layers, columns)) == 1, speed_ref[0], LAND
    )
    square = (group, group)
    diagonal = lax.broadcasted_iota(jnp.int32, square, 0) == lax.broadcasted_iota(
        jnp.int32, square, 1
    )
    settle = jnp.sum(jnp.where(diagonal, settling_ref[...], 0.0), axis=1, keepdims=True)
    settle = jnp.broadcast_to(settle, (group, CY))

    def line_up(x):
        for l in range(layers):
            for j in range(CY // LANES):
                field_ref[strip(l), x * CY + j * LANES : x * CY + (j + 1) * LANES] = flat_ref[
                    pl.ds(x * block + j * layers + l, group, stride=tile_lanes * layers), :
                ]

    def enter():
        before = lax.div(tile + tiles - 1, tiles)
        after = lax.div(2 * (tiles - 1) - tile, tiles)
        pl.semaphore_wait(barrier, peers - 1 + before + after)

    far_side = lax.rem(tile, 2)
    sides = (far_side, 1 - far_side)
    edges = [side * (CX - 1) for side in sides]

    def there(way):
        side = sides[way]
        return (1 - side) * tile + side * (tiles - 1 - tile) > 0

    lonely = 1 - lax.div(tile + tiles - 1, tiles) * lax.div(2 * (tiles - 1) - tile, tiles)

    def beyond(way):
        return {"tile": tile - 1 + 2 * sides[way]}

    def drift(way):
        side = sides[way]
        return pltpu.make_async_remote_copy(
            src_ref=drift_ref.at[:, cols(edges[way] + 1)],
            dst_ref=drift_ref.at[:, cols((1 - side) * (CX + 1))],
            send_sem=load_sem.at[way],
            recv_sem=drift_recv.at[way],
            device_id=beyond(way),
            device_id_type=MESH,
        )

    def halo(way, h):
        return pltpu.make_async_remote_copy(
            src_ref=field_ref.at[:, span(edges[way] * CY + h * UNIT, UNIT)],
            dst_ref=halo_ref.at[way, :, pl.ds(h * UNIT, UNIT)],
            send_sem=load_sem.at[2 + way],
            recv_sem=halo_recv.at[way, h],
            device_id=beyond(way),
            device_id_type=MESH,
        )

    def reach_out():
        for way in range(2):

            @pl.when(there(way))
            def _():
                drift(way).start()
                for h in range(SPLIT):
                    halo(way, h).start()

    def await_all(ref, sem):
        pltpu.make_async_copy(ref, ref, sem).wait()

    def arrival(u):
        inner = (u - SPLIT) // SPLIT + SPLIT
        return u if u < SPLIT else inner if u < (CX - 1) * SPLIT else u - (CX - 2) * (SPLIT - 1)

    def forward(n, u, start, width, s):
        at = span(start, width)
        return pltpu.make_async_remote_copy(
            src_ref=moved_ref.at[partners[n] * own + s, :, at],
            dst_ref=whole_ref.at[s, span(me * group, group), at],
            send_sem=out_send,
            recv_sem=out_recv.at[arrival(u), s],
            device_id={"cls": partners[n]},
            device_id_type=MESH,
        )

    def send(u, start, width):
        for s in range(own):
            for n in range(peers - 1):
                forward(n, u, start, width, s).start()
        at = span(start, width)
        for s in range(own):
            whole_ref[s, span(me * group, group), at] = moved_ref[me * own + s, :, at]

    def backward(n, u, start, width, s):
        at = span(start, width)
        return pltpu.make_async_remote_copy(
            src_ref=done_ref.at[s, span(partners[n] * group, group), at],
            dst_ref=back_ref.at[me * own + s, :, at],
            send_sem=load_sem.at[4],
            recv_sem=back_recv.at[u],
            device_id={"cls": partners[n]},
            device_id_type=MESH,
        )

    def transport(x, way=None):
        def row(at):
            value = drift_ref[:, cols(at)]
            return value, jnp.where(value < 0.5 * LAND, 1.0, 0.0)

        speed, water = row(x + 1)
        speed_low, water_low = row(x)
        speed_high, water_high = row(x + 2)
        face_low = 0.5 * (speed_low + speed) * (water_low * water)
        face_high = 0.5 * (speed + speed_high) * (water * water_high)
        v = speed_ref[1, :, cols(x)]
        lane = lax.broadcasted_iota(jnp.int32, v.shape, 1)
        side_high = 0.5 * (v + pltpu.roll(v, CY - 1, 1)) * (water * pltpu.roll(water, CY - 1, 1))
        side_high = jnp.where(lane == CY - 1, 0.0, side_high)
        side_low = pltpu.roll(side_high, 1, 1)
        up = jnp.maximum
        down = jnp.minimum
        centre = (
            1.0 - up(face_high, 0.0) + down(face_low, 0.0) - up(side_high, 0.0) + down(side_low, 0.0)
        )
        west = up(face_low, 0.0)
        east = -down(face_high, 0.0)
        south = up(side_low, 0.0)
        north = -down(side_high, 0.0)
        if way is None:
            inner = ((west, x - 1), (east, x + 1))
        else:
            eastern = sides[way] == 1
            outer_ref[way] = jnp.where(eastern, east, west)
            inner = ((jnp.where(eastern, west, east), x + 1 - 2 * sides[way]),)
        for l in range(layers):
            c = field_ref[strip(l), cols(x)]
            moved = (
                (centre[l : l + 1] - settle) * c
                + south[l : l + 1] * pltpu.roll(c, 1, 1)
                + north[l : l + 1] * pltpu.roll(c, CY - 1, 1)
            )
            for factor, at in inner:
                moved = moved + factor[l : l + 1] * field_ref[strip(l), cols(at)]
            if l > 0:
                moved = moved + settle * field_ref[strip(l - 1), cols(x)]
            moved_ref[l, :, cols(x)] = moved

    rows = CX - 2

    def prepare(way):
        @pl.when(there(way))
        def _():
            with jax.named_scope(f'driftwait{way}'):
                drift(way).wait_recv()

        transport(edges[way], way)

    def close(way, h):
        start = edges[way] * CY + h * UNIT

        @pl.when(there(way))
        def _():
            with jax.named_scope(f'halowait{way}'):
                halo(way, h).wait_recv()
            at = pl.ds(h * UNIT, UNIT)
            for l in range(layers):
                moved_ref[l, :, span(start, UNIT)] += (
                    outer_ref[way, l : l + 1, at] * halo_ref[way, strip(l), at]
                )

        send((rows + way) * SPLIT + h, start, UNIT)

    def send_row(x):
        for h in range(SPLIT):
            send((x - 1) * SPLIT + h, x * CY + h * UNIT, UNIT)

    for x in range(CX):
        line_up(x)
    transport(1)
    enter()
    reach_out()
    send_row(1)
    for x in range(2, CX - 1):
        transport(x)
        send_row(x)

    loads[4].wait()
    await_all(table_ref, load_sem.at[len(loads)])
    build_tables(table_ref.at[0], table_ref.at[1], table_ref.at[2], rate_ref, quad_ref, pair_ref)

    @pl.when(jnp.logical_not(there(0)))
    def _():
        prepare(0)
        for h in range(SPLIT):
            close(0, h)

    def slot(k):
        row = k // SPLIT
        return 0 if row < CX - 2 else row - (CX - 3) + (k % SPLIT if row == CX - 1 else 0)

    def unit(u, start, width):
        at = span(start, width)
        for s in range(own):
            await_all(whole_ref.at[s, pl.ds(0, (peers - 1) * group), at], out_recv.at[arrival(u), s])
            now = react(whole_ref[s, :, at], quad_ref, pair_ref)
            done_ref[s, :, at] = react(now, quad_ref, pair_ref)
            back_ref[me * own + s, :, at] = done_ref[s, span(me * group, group), at]

    def start_of(k):
        q, h = divmod(k, SPLIT)
        return (q + 1 if q < rows else edges[q - rows]) * CY + h * UNIT

    def give_back(k):
        for s in range(own):
            for n in range(peers - 1):
                backward(n, slot(k), start_of(k), UNIT, s).start()

    def act(name):
        kind, *rest = name
        if kind == "unit":
            k, wide = rest
            unit(k, start_of(k), CY if wide else UNIT)
        elif kind == "back":
            give_back(rest[0])
        elif kind == "far":
            @pl.when(there(0))
            def _():
                prepare(0) if rest[0] == "prep" else close(0, rest[0])
        else:
            @pl.when(lonely == (1 if kind == "alone" else 0))
            def _():
                prepare(1) if rest[0] == "prep" else close(1, rest[0])

    for name in PLAN:
        act(name)

    for way in range(2):

        @pl.when(there(way))
        def _():
            drift(way).wait_send()
            await_all(halo_ref.at[way], load_sem.at[2 + way])

    def ahead(start, width):
        return pl.ds(pl.multiple_of(start, UNIT), width)

    def finish(u, start, width):
        await_all(
            back_ref.at[pl.ds(0, (peers - 1) * own), :, ahead(start, width)], back_recv.at[u]
        )
        for l in range(layers):
            for j in range(width // LANES):
                at = (lax.div(start, LANES) + j) * layers + l
                out_ref[pl.ds(at, group, stride=tile_lanes * layers), :] = back_ref[
                    l, :, span(start + j * LANES, LANES)
                ]

    await_all(moved_ref.at[pl.ds(0, (peers - 1) * own)], out_send)
    finish(0, CY, rows * CY)
    finish(1, edges[0] * CY, CY)
    for h in range(SPLIT):
        finish(2 + h, edges[1] * CY + h * UNIT, UNIT)
    await_all(done_ref.at[:, pl.ds(0, (peers - 1) * group), :], load_sem.at[4])


PLAN = (
    ("unit", 0, 0),
    ("back", 0),
    ("far", "prep"),
    ("far", 0),
    ("unit", 1, 0),
    ("far", 1),
    ("back", 1),
    ("alone", "prep"),
    ("alone", 0),
    ("alone", 1),
    ("unit", 2, 1),
    ("near", "prep"),
    ("near", 0),
    ("back", 2),
    ("near", 1),
    ("back", 3),
    ("unit", 4, 1),
    ("back", 4),
    ("back", 5),
    ("unit", 6, 0),
    ("back", 6),
    ("unit", 7, 0),
    ("back", 7),
)


def body(
    tiles,
    peers,
    concentration,
    velocity,
    land_mask,
    settling,
    breakage_rate,
    kernel_levels,
    pair_target,
    fragment_weights,
):
    group, layers, columns = concentration.shape
    total = kernel_levels.shape[0]
    own = layers // peers
    flat = concentration.reshape(group, layers, columns // LANES, LANES)
    flat = jnp.transpose(flat, (0, 2, 1, 3)).reshape(-1, LANES)
    operands = (
        flat,
        velocity,
        land_mask.reshape(1, columns),
        settling.reshape(1, group),
        breakage_rate.reshape(1, total),
        kernel_levels,
        pair_target,
        fragment_weights,
    )
    dma = pltpu.SemaphoreType.DMA
    done = pl.pallas_call(
        functools.partial(step_kernel, tiles, peers),
        out_shape=pltpu.VMEM((group * layers * columns // LANES, LANES), jnp.float32),
        in_specs=[pl.BlockSpec(memory_space=pl.ANY)] * len(operands),
        out_specs=pl.BlockSpec(memory_space=pltpu.VMEM),
        scratch_shapes=[
            *[pltpu.VMEM(x.shape, x.dtype) for x in operands[:5]],
            pltpu.VMEM((3, total, total), jnp.int32),
            pltpu.VMEM((quad_rows(total), 4 * total), jnp.bfloat16),
            pltpu.VMEM((2 * total, pair_rows() + total), jnp.bfloat16),
            pltpu.VMEM((layers * group, columns), jnp.float32),
            pltpu.VMEM((layers, columns + 2 * CY), jnp.float32),
            pltpu.VMEM((2, layers, CY), jnp.float32),
            pltpu.VMEM((2, layers * group, CY), jnp.float32),
            pltpu.VMEM((layers, group, columns), jnp.float32),
            pltpu.VMEM((own, total, columns), jnp.float32),
            pltpu.VMEM((own, total, columns), jnp.float32),
            pltpu.VMEM((layers, group, columns), jnp.float32),
            dma((6,)),
            dma((2,)),
            dma((2, SPLIT)),
            dma,
            dma((UNITS, own)),
            dma((CX - 2 + SPLIT,)),
        ],
        compiler_params=pltpu.CompilerParams(collective_id=0, has_side_effects=True),
    )(*operands)
    done = done.reshape(group, columns // LANES, layers, LANES)
    return jnp.transpose(done, (0, 2, 1, 3)).reshape(group, layers, columns)


def solution(mesh):
    return jax.shard_map(
        functools.partial(body, mesh.shape["tile"], mesh.shape["cls"]),
        mesh=mesh,
        in_specs=(
            P("cls", None, "tile"),
            P(None, None, "tile"),
            P("tile"),
            P("cls"),
            P(),
            P(),
            P(),
            P(),
        ),
        out_specs=P("cls", None, "tile"),
        check_vma=False,
    )
```

```python
import functools

import jax
import jax.numpy as jnp
from jax import lax
from jax.experimental import pallas as pl
from jax.experimental.pallas import tpu as pltpu
from jax.sharding import PartitionSpec as P

CY = 512
CX = 4
half_scale = 0.5e-05
STEP = 8
EDGE = 16
LARGEST = 448
LANES = 128
SPLIT = 2
UNIT = CY // SPLIT
UNITS = CX - 2 + 2 * SPLIT


def split_pair(value, lane, total):
    high = value.astype(jnp.bfloat16).astype(jnp.float32)
    return jnp.where(lane < total, high, value - high).astype(jnp.bfloat16)


def halves(value):
    high = value.astype(jnp.bfloat16)
    return high, (value - high.astype(jnp.float32)).astype(jnp.bfloat16)


def pair_span(i):
    return STEP * (i // STEP + 1)


def quad_rows(total):
    return sum(STEP * (total - first) for first in range(EDGE, total, STEP)) + EDGE


def pair_rows():
    return sum(pair_span(i) for i in range(EDGE))


def build_tables(levels_ref, target_ref, weights_ref, rate_ref, quad_ref, pair_ref):
    total = levels_ref.shape[0]
    wide = 2 * total
    narrow = levels_ref[...].astype(jnp.float32)
    levels = jnp.concatenate([narrow, narrow], 1)
    target = target_ref[...]
    target = jnp.concatenate([target, target], 1)
    row = lax.broadcasted_iota(jnp.int32, (total, wide), 0)
    lane = lax.broadcasted_iota(jnp.int32, (total, wide), 1)
    col = jnp.where(lane < total, lane, lane - total)
    twice = 2.0 * levels
    birth = jnp.where(col < row, twice, jnp.where(col == row, levels, 0.0))

    def put(offset, value, lane):
        count = value.shape[0]
        packed = split_pair(value, lane, total)
        quad_ref[offset : offset + count, :wide] = packed
        quad_ref[offset : offset + count, wide:] = packed
        return offset + count

    offset = 0
    for first in range(EDGE, total, STEP):
        rank = row[first:]
        for i in range(first, first + STEP):
            value = jnp.where(target[i : i + 1] == rank, birth[i : i + 1], 0.0)
            value = value - jnp.where(rank == i, twice[i : i + 1], 0.0)
            offset = put(offset, value, lane[first:])
    put(offset, jnp.where(col[:EDGE] >= EDGE, twice[:EDGE], 0.0), lane[:EDGE])

    count = pair_rows()

    def flat(make):
        return jnp.concatenate([make(i, pair_span(i)) for i in range(EDGE)], 1)

    rank = lax.broadcasted_iota(jnp.int32, (total, count), 0)
    one = flat(lambda i, width: jnp.full((1, width), i, jnp.int32))
    other = flat(lambda i, width: lax.broadcasted_iota(jnp.int32, (1, width), 1))
    goal = flat(lambda i, width: target_ref[i : i + 1, :width])
    level = flat(lambda i, width: 2.0 * levels_ref[i : i + 1, :width].astype(jnp.float32))
    level = jnp.where(other <= one, level, 0.0)
    same = other == one
    value = jnp.where(rank == goal, jnp.where(same, 0.5 * level, level), 0.0)
    value = value - jnp.where(rank == one, level, 0.0)
    value = value - jnp.where(rank == other, jnp.where(same, 0.0, level), 0.0)
    square = (total, total)
    row = lax.broadcasted_iota(jnp.int32, square, 0)
    col = lax.broadcasted_iota(jnp.int32, square, 1)
    lower = jnp.where(row <= col, weights_ref[...].astype(jnp.float32), 0.0)
    frag = lower / jnp.sum(lower, axis=0, keepdims=True)
    rate = rate_ref[...]
    linear = (frag * rate - jnp.where(row == col, rate, 0.0)) * (1.0 / half_scale)
    high, low = halves(jnp.concatenate([value, linear], 1))
    pair_ref[:total] = high
    pair_ref[total:] = low


def react(now, quad_ref, pair_ref):
    total = now.shape[0]
    high, low = halves(now)
    stack = jnp.concatenate([high, high, low, low], 0)
    ahead = [now[: pair_span(i)] * now[i : i + 1] for i in range(EDGE)]
    high, low = halves(jnp.concatenate([*ahead, now], 0))

    def dot(table, value):
        return jnp.dot(table, value, preferred_element_type=jnp.float32)

    spans = [(first, STEP * (total - first)) for first in range(EDGE, total, STEP)] + [(None, EDGE)]
    made = {}
    offset = 0
    while spans:
        taken = [spans.pop(0)]
        while spans and sum(count for _, count in taken) + spans[0][1] <= LARGEST:
            taken.append(spans.pop(0))
        count = sum(count for _, count in taken)
        product = dot(quad_ref[offset : offset + count, :], stack)
        offset += count
        start = 0
        for first, count in taken:
            made[first] = product[start : start + count]
            start += count

    gain = None
    for first in range(EDGE, total, STEP):
        count = total - first
        part = made[first][:count] * now[first : first + 1]
        for r in range(1, STEP):
            part = part + made[first][r * count : (r + 1) * count] * now[first + r : first + r + 1]
        skip = first - EDGE
        gain = part if gain is None else jnp.concatenate([gain[:skip], gain[skip:] + part], 0)
    loss = made[None] * now[:EDGE]
    both = dot(pair_ref[...], high)
    rest = both[:total] + both[total:] + dot(pair_ref[:total], low)
    return now + (rest + jnp.concatenate([-loss, gain], 0)) * half_scale


MESH = pl.DeviceIdType.MESH
LAND = 4.0


def step_kernel(
    tiles,
    peers,
    flat_hbm,
    speed_hbm,
    water_hbm,
    settling_hbm,
    rate_hbm,
    levels_hbm,
    target_hbm,
    weights_hbm,
    out_ref,
    speed_ref,
    water_ref,
    settling_ref,
    rate_ref,
    table_ref,
    quad_ref,
    pair_ref,
    field_ref,
    drift_ref,
    outer_ref,
    halo_ref,
    moved_ref,
    whole_ref,
    done_ref,
    back_ref,
    twin_ref,
    twin_done_ref,
    load_sem,
    drift_recv,
    halo_recv,
    out_send,
    out_recv,
    back_recv,
    twin_sem,
):
    layers, group, columns = moved_ref.shape
    tile_lanes = columns // LANES
    block = CY // LANES * layers
    own = layers // peers
    tile = lax.axis_index("tile")
    me = lax.axis_index("cls")
    has_west = tile > 0
    has_east = tile < tiles - 1

    if peers == 4:
        partners = [lax.rem(me + 2, 4), 3 - me, me + 1 - 2 * lax.rem(me, 2)]
    else:
        partners = [lax.rem(me + d, peers) for d in range(1, peers)]

    twin = lax.rem(me + peers // 2, peers)
    beside = peers - 2

    barrier = pltpu.get_barrier_semaphore()

    @pl.when(has_west)
    def _():
        pl.semaphore_signal(barrier, inc=1, device_id={"tile": tile - 1}, device_id_type=MESH)

    @pl.when(has_east)
    def _():
        pl.semaphore_signal(barrier, inc=1, device_id={"tile": tile + 1}, device_id_type=MESH)

    for p in partners:
        pl.semaphore_signal(barrier, inc=1, device_id={"cls": p}, device_id_type=MESH)

    loads = [
        pltpu.make_async_copy(source, place, load_sem.at[n + 1])
        for n, (source, place) in enumerate(
            (
                (speed_hbm, speed_ref),
                (water_hbm, water_ref),
                (settling_hbm, settling_ref),
                (rate_hbm, rate_ref),
            )
        )
    ]
    for copy in loads[:3]:
        copy.start()
    for x in range(CX):
        for j in range(x * (CY // LANES), (x + 1) * (CY // LANES)):
            for l in range(layers):
                pltpu.make_async_copy(
                    flat_hbm.at[:, j * layers + l, 0, :],
                    field_ref.at[pl.ds(l * group, group), pl.ds(j * LANES, LANES)],
                    load_sem.at[0 if x < CX - 1 else 6],
                ).start()
    for copy in loads[3:]:
        copy.start()
    for n, source in enumerate((levels_hbm, target_hbm, weights_hbm)):
        pltpu.make_async_copy(source, table_ref.at[n], load_sem.at[len(loads) + 1]).start()

    def await_all(ref, sem):
        pltpu.make_async_copy(ref, ref, sem).wait()

    def span(start, width):
        return pl.ds(pl.multiple_of(start, width), width)

    def cols(x):
        return span(x * CY, CY)

    def strip(l):
        return pl.ds(l * group, group)

    for side, exists in ((0, has_west), (1, has_east)):

        @pl.when(jnp.logical_not(exists))
        def _():
            drift_ref[:, cols(side * (CX + 1))] = jnp.full((layers, CY), LAND, jnp.float32)

    for copy in loads[:3]:
        copy.wait()
    drift_ref[:, pl.ds(CY, columns)] = jnp.where(
        jnp.broadcast_to(water_ref[...], (layers, columns)) == 1, speed_ref[0], LAND
    )
    square = (group, group)
    diagonal = lax.broadcasted_iota(jnp.int32, square, 0) == lax.broadcasted_iota(
        jnp.int32, square, 1
    )
    settle = jnp.sum(jnp.where(diagonal, settling_ref[...], 0.0), axis=1, keepdims=True)
    settle = jnp.broadcast_to(settle, (group, CY))

    def enter():
        before = lax.div(tile + tiles - 1, tiles)
        after = lax.div(2 * (tiles - 1) - tile, tiles)
        pl.semaphore_wait(barrier, peers - 1 + before + after)

    far_side = lax.rem(tile, 2)
    sides = (far_side, 1 - far_side)
    edges = [side * (CX - 1) for side in sides]

    def there(way):
        side = sides[way]
        return (1 - side) * tile + side * (tiles - 1 - tile) > 0

    lonely = 1 - lax.div(tile + tiles - 1, tiles) * lax.div(2 * (tiles - 1) - tile, tiles)

    def beyond(way):
        return {"tile": tile - 1 + 2 * sides[way]}

    def drift(way):
        side = sides[way]
        return pltpu.make_async_remote_copy(
            src_ref=drift_ref.at[:, cols(edges[way] + 1)],
            dst_ref=drift_ref.at[:, cols((1 - side) * (CX + 1))],
            send_sem=load_sem.at[way],
            recv_sem=drift_recv.at[way],
            device_id=beyond(way),
            device_id_type=MESH,
        )

    def halo(way, h):
        return pltpu.make_async_remote_copy(
            src_ref=field_ref.at[:, span(edges[way] * CY + h * UNIT, UNIT)],
            dst_ref=halo_ref.at[way, :, pl.ds(h * UNIT, UNIT)],
            send_sem=load_sem.at[2 + way],
            recv_sem=halo_recv.at[way, h],
            device_id=beyond(way),
            device_id_type=MESH,
        )

    def reach_out():
        for way in range(2):

            @pl.when(there(way))
            def _():
                drift(way).start()
                for h in range(SPLIT):
                    halo(way, h).start()

    def arrival(u):
        inner = (u - SPLIT) // SPLIT + SPLIT
        return u if u < SPLIT else inner if u < (CX - 1) * SPLIT else u - (CX - 2) * (SPLIT - 1)

    def forward(n, u, start, width, s):
        at = span(start, width)
        return pltpu.make_async_remote_copy(
            src_ref=moved_ref.at[partners[n] * own + s, :, at],
            dst_ref=whole_ref.at[s, span(me * group, group), at],
            send_sem=out_send,
            recv_sem=out_recv.at[arrival(u), s],
            device_id={"cls": partners[n]},
            device_id_type=MESH,
        )

    def send(u, start, width):
        for s in range(own):
            for n in range(peers - 1):
                forward(n, u, start, width, s).start()
        at = span(start, width)
        for s in range(own):
            whole_ref[s, span(me * group, group), at] = moved_ref[me * own + s, :, at]

    rows = CX - 2

    def slot(k):
        row = k // SPLIT
        return row + (k % SPLIT if row == CX - 1 else 0)

    def backward(n, k, start, width, s):
        at = span(start, width)
        return pltpu.make_async_remote_copy(
            src_ref=done_ref.at[s, span(partners[n] * group, group), at],
            dst_ref=back_ref.at[me * own + s, :, at],
            send_sem=twin_sem.at[2] if k // SPLIT == rows - 1 else load_sem.at[4],
            recv_sem=back_recv.at[slot(k)],
            device_id={"cls": partners[n]},
            device_id_type=MESH,
        )

    def transport(x, way=None):
        def row(at):
            value = drift_ref[:, cols(at)]
            return value, jnp.where(value < 0.5 * LAND, 1.0, 0.0)

        speed, water = row(x + 1)
        speed_low, water_low = row(x)
        speed_high, water_high = row(x + 2)
        face_low = 0.5 * (speed_low + speed) * (water_low * water)
        face_high = 0.5 * (speed + speed_high) * (water * water_high)
        v = speed_ref[1, :, cols(x)]
        lane = lax.broadcasted_iota(jnp.int32, v.shape, 1)
        side_high = 0.5 * (v + pltpu.roll(v, CY - 1, 1)) * (water * pltpu.roll(water, CY - 1, 1))
        side_high = jnp.where(lane == CY - 1, 0.0, side_high)
        side_low = pltpu.roll(side_high, 1, 1)
        up = jnp.maximum
        down = jnp.minimum
        centre = (
            1.0 - up(face_high, 0.0) + down(face_low, 0.0) - up(side_high, 0.0) + down(side_low, 0.0)
        )
        west = up(face_low, 0.0)
        east = -down(face_high, 0.0)
        south = up(side_low, 0.0)
        north = -down(side_high, 0.0)
        if way is None:
            inner = ((west, x - 1), (east, x + 1))
        else:
            eastern = sides[way] == 1
            outer_ref[way] = jnp.where(eastern, east, west)
            inner = ((jnp.where(eastern, west, east), x + 1 - 2 * sides[way]),)
        for l in range(layers):
            c = field_ref[strip(l), cols(x)]
            moved = (
                (centre[l : l + 1] - settle) * c
                + south[l : l + 1] * pltpu.roll(c, 1, 1)
                + north[l : l + 1] * pltpu.roll(c, CY - 1, 1)
            )
            for factor, at in inner:
                moved = moved + factor[l : l + 1] * field_ref[strip(l), cols(at)]
            if l > 0:
                moved = moved + settle * field_ref[strip(l - 1), cols(x)]
            moved_ref[l, :, cols(x)] = moved

    def prepare(way):
        @pl.when(there(way))
        def _():
            drift(way).wait_recv()

        transport(edges[way], way)

    def close(way, h):
        start = edges[way] * CY + h * UNIT

        @pl.when(there(way))
        def _():
            halo(way, h).wait_recv()
            at = pl.ds(h * UNIT, UNIT)
            for l in range(layers):
                moved_ref[l, :, span(start, UNIT)] += (
                    outer_ref[way, l : l + 1, at] * halo_ref[way, strip(l), at]
                )

        send((rows + way) * SPLIT + h, start, UNIT)

    double = there(0) if peers == 4 else False
    middle = cols(CX - 2)

    def extra(n, s):
        return pltpu.make_async_remote_copy(
            src_ref=moved_ref.at[lax.rem(partners[n] + peers // 2, peers) * own + s, :, middle],
            dst_ref=twin_ref.at[s, span(me * group, group)],
            send_sem=twin_sem.at[0],
            recv_sem=twin_sem.at[1],
            device_id={"cls": partners[n]},
            device_id_type=MESH,
        )

    def send_twice():
        for s in range(own):
            for n in range(peers - 1):
                extra(n, s).start()
            twin_ref[s, span(me * group, group)] = moved_ref[twin * own + s, :, middle]

    def twin_back(s):
        return pltpu.make_async_remote_copy(
            src_ref=twin_done_ref.at[s, span(partners[beside] * group, group)],
            dst_ref=back_ref.at[twin * own + s, :, middle],
            send_sem=twin_sem.at[2],
            recv_sem=back_recv.at[rows - 1],
            device_id={"cls": partners[beside]},
            device_id_type=MESH,
        )

    def twin_unit():
        await_all(twin_ref.at[:, pl.ds(0, (peers - 1) * group)], twin_sem.at[1])
        for s in range(own):
            now = react(twin_ref[s], quad_ref, pair_ref)
            twin_done_ref[s] = react(now, quad_ref, pair_ref)
            twin_back(s).start()
            back_ref[twin * own + s, :, middle] = twin_done_ref[s, span(me * group, group)]

    def send_row(x):
        for h in range(SPLIT):
            send((x - 1) * SPLIT + h, x * CY + h * UNIT, UNIT)

    inner = pl.ds(0, (CX - 1) * CY)
    await_all(field_ref.at[:, inner], load_sem.at[0])
    transport(1)
    enter()
    send_row(1)
    await_all(field_ref.at[:, cols(CX - 1)], load_sem.at[6])
    reach_out()
    for x in range(2, CX - 1):
        transport(x)
        send_row(x)

    @pl.when(double)
    def _():
        send_twice()

    loads[3].wait()
    await_all(table_ref, load_sem.at[len(loads) + 1])
    build_tables(table_ref.at[0], table_ref.at[1], table_ref.at[2], rate_ref, quad_ref, pair_ref)

    @pl.when(jnp.logical_not(there(0)))
    def _():
        prepare(0)
        for h in range(SPLIT):
            close(0, h)

    def unit(u, start, width):
        at = span(start, width)
        for s in range(own):
            await_all(whole_ref.at[s, pl.ds(0, (peers - 1) * group), at], out_recv.at[arrival(u), s])
            now = react(whole_ref[s, :, at], quad_ref, pair_ref)
            done_ref[s, :, at] = react(now, quad_ref, pair_ref)
            back_ref[me * own + s, :, at] = done_ref[s, span(me * group, group), at]

    def start_of(k):
        q, h = divmod(k, SPLIT)
        return (q + 1 if q < rows else edges[q - rows]) * CY + h * UNIT

    def give_back(k):
        for s in range(own):
            for n in range(peers - 1):
                backward(n, k, start_of(k), UNIT, s).start()

    def act(name):
        kind, *rest = name
        if kind == "unit":
            k, wide = rest
            unit(k, start_of(k), CY if wide else UNIT)
        elif kind == "back":
            if rest[0] // SPLIT == rows - 1:
                pl.when(jnp.logical_not(double))(lambda: give_back(rest[0]))
            else:
                give_back(rest[0])
        elif kind == "beside":
            @pl.when(double)
            def _():
                for s in range(own):
                    for h in range(SPLIT):
                        k = (rows - 1) * SPLIT + h
                        backward(beside, k, start_of(k), UNIT, s).start()
        elif kind == "twin":
            pl.when(double)(twin_unit)
        elif kind == "far":
            @pl.when(there(0))
            def _():
                prepare(0) if rest[0] == "prep" else close(0, rest[0])
        else:
            @pl.when(lonely == (1 if kind == "alone" else 0))
            def _():
                prepare(1) if rest[0] == "prep" else close(1, rest[0])

    for name in PLAN:
        act(name)

    for way in range(2):

        @pl.when(there(way))
        def _():
            drift(way).wait_send()
            await_all(halo_ref.at[way], load_sem.at[2 + way])

    def settle_out(start, width):
        for l in range(layers):
            for j in range(width // LANES):
                at = (lax.div(start, LANES) + j) * layers + l
                out_ref[pl.ds(at, group, stride=tile_lanes * layers), :] = back_ref[
                    l, :, span(start + j * LANES, LANES)
                ]

    def finish(u, start, width):
        await_all(
            back_ref.at[pl.ds(0, (peers - 1) * own), :, span(start, width)], back_recv.at[u]
        )
        settle_out(start, width)

    await_all(moved_ref.at[pl.ds(0, (peers - 1) * own)], out_send)
    for q in range(rows - 1):
        finish(q, (q + 1) * CY, CY)

    @pl.when(double)
    def _():
        await_all(twin_ref.at[:, pl.ds(0, (peers - 1) * group)], twin_sem.at[0])
        await_all(twin_ref.at[:, pl.ds(0, 2 * group)], twin_sem.at[2])
        await_all(back_ref.at[pl.ds(0, 2 * own), :, middle], back_recv.at[rows - 1])

    @pl.when(jnp.logical_not(double))
    def _():
        await_all(done_ref.at[:, pl.ds(0, (peers - 1) * group), middle], twin_sem.at[2])
        await_all(back_ref.at[pl.ds(0, (peers - 1) * own), :, middle], back_recv.at[rows - 1])

    settle_out((CX - 2) * CY, CY)
    finish(rows, edges[0] * CY, CY)
    for h in range(SPLIT):
        finish(rows + 1 + h, edges[1] * CY + h * UNIT, UNIT)
    await_all(done_ref.at[:, pl.ds(0, (peers - 1) * group), pl.ds(0, (CX - 1) * CY)], load_sem.at[4])


PLAN = (
    ("unit", 0, 0),
    ("back", 0),
    ("far", "prep"),
    ("far", 0),
    ("unit", 1, 0),
    ("far", 1),
    ("back", 1),
    ("alone", "prep"),
    ("alone", 0),
    ("alone", 1),
    ("unit", 2, 1),
    ("beside",),
    ("back", 2),
    ("back", 3),
    ("near", "prep"),
    ("near", 0),
    ("twin",),
    ("near", 1),
    ("unit", 4, 1),
    ("back", 4),
    ("back", 5),
    ("unit", 6, 0),
    ("back", 6),
    ("unit", 7, 0),
    ("back", 7),
)


def body(
    tiles,
    peers,
    concentration,
    velocity,
    land_mask,
    settling,
    breakage_rate,
    kernel_levels,
    pair_target,
    fragment_weights,
):
    group, layers, columns = concentration.shape
    total = kernel_levels.shape[0]
    own = layers // peers
    flat = concentration.reshape(group, layers, columns // LANES, LANES)
    flat = jnp.transpose(flat, (0, 2, 1, 3)).reshape(group, -1, 1, LANES)
    operands = (
        flat,
        velocity,
        land_mask.reshape(1, columns),
        settling.reshape(1, group),
        breakage_rate.reshape(1, total),
        kernel_levels,
        pair_target,
        fragment_weights,
    )
    dma = pltpu.SemaphoreType.DMA
    done = pl.pallas_call(
        functools.partial(step_kernel, tiles, peers),
        out_shape=pltpu.VMEM((group * layers * columns // LANES, LANES), jnp.float32),
        in_specs=[pl.BlockSpec(memory_space=pl.ANY)] * len(operands),
        out_specs=pl.BlockSpec(memory_space=pltpu.VMEM),
        scratch_shapes=[
            *[pltpu.VMEM(x.shape, x.dtype) for x in operands[1:5]],
            pltpu.VMEM((3, total, total), jnp.int32),
            pltpu.VMEM((quad_rows(total), 4 * total), jnp.bfloat16),
            pltpu.VMEM((2 * total, pair_rows() + total), jnp.bfloat16),
            pltpu.VMEM((layers * group, columns), jnp.float32),
            pltpu.VMEM((layers, columns + 2 * CY), jnp.float32),
            pltpu.VMEM((2, layers, CY), jnp.float32),
            pltpu.VMEM((2, layers * group, CY), jnp.float32),
            pltpu.VMEM((layers, group, columns), jnp.float32),
            pltpu.VMEM((own, total, columns), jnp.float32),
            pltpu.VMEM((own, total, columns), jnp.float32),
            pltpu.VMEM((layers, group, columns), jnp.float32),
            pltpu.VMEM((own, total, CY), jnp.float32),
            pltpu.VMEM((own, total, CY), jnp.float32),
            dma((7,)),
            dma((2,)),
            dma((2, SPLIT)),
            dma,
            dma((UNITS, own)),
            dma((CX - 1 + SPLIT,)),
            dma((3,)),
        ],
        compiler_params=pltpu.CompilerParams(collective_id=0, has_side_effects=True),
    )(*operands)
    done = done.reshape(group, columns // LANES, layers, LANES)
    return jnp.transpose(done, (0, 2, 1, 3)).reshape(group, layers, columns)


def solution(mesh):
    return jax.shard_map(
        functools.partial(body, mesh.shape["tile"], mesh.shape["cls"]),
        mesh=mesh,
        in_specs=(
            P("cls", None, "tile"),
            P(None, None, "tile"),
            P("tile"),
            P("cls"),
            P(),
            P(),
            P(),
            P(),
        ),
        out_specs=P("cls", None, "tile"),
        check_vma=False,
    )
```

```python
import functools

import jax
import jax.numpy as jnp
from jax import lax
from jax.experimental import pallas as pl
from jax.experimental.pallas import tpu as pltpu
from jax.sharding import PartitionSpec as P

CY = 512
CX = 4
half_scale = 0.5e-05
STEP = 8
EDGE = 16
LARGEST = 448
LANES = 128
SPLIT = 2
UNIT = CY // SPLIT
UNITS = CX - 2 + 2 * SPLIT


def split_pair(value, lane, total):
    high = value.astype(jnp.bfloat16).astype(jnp.float32)
    return jnp.where(lane < total, high, value - high).astype(jnp.bfloat16)


def halves(value):
    high = value.astype(jnp.bfloat16)
    return high, (value - high.astype(jnp.float32)).astype(jnp.bfloat16)


def pair_span(i):
    return STEP * (i // STEP + 1)


def quad_rows(total):
    return sum(STEP * (total - first) for first in range(EDGE, total, STEP)) + EDGE


def pair_rows():
    return sum(pair_span(i) for i in range(EDGE))


def build_tables(levels_ref, target_ref, weights_ref, rate_ref, quad_ref, pair_ref):
    total = levels_ref.shape[0]
    wide = 2 * total
    narrow = levels_ref[...].astype(jnp.float32)
    levels = jnp.concatenate([narrow, narrow], 1)
    target = target_ref[...]
    target = jnp.concatenate([target, target], 1)
    row = lax.broadcasted_iota(jnp.int32, (total, wide), 0)
    lane = lax.broadcasted_iota(jnp.int32, (total, wide), 1)
    col = jnp.where(lane < total, lane, lane - total)
    twice = 2.0 * levels
    birth = jnp.where(col < row, twice, jnp.where(col == row, levels, 0.0))

    def put(offset, value, lane):
        count = value.shape[0]
        packed = split_pair(value, lane, total)
        quad_ref[offset : offset + count, :wide] = packed
        quad_ref[offset : offset + count, wide:] = packed
        return offset + count

    offset = 0
    for first in range(EDGE, total, STEP):
        rank = row[first:]
        for i in range(first, first + STEP):
            value = jnp.where(target[i : i + 1] == rank, birth[i : i + 1], 0.0)
            value = value - jnp.where(rank == i, twice[i : i + 1], 0.0)
            offset = put(offset, value, lane[first:])
    put(offset, jnp.where(col[:EDGE] >= EDGE, twice[:EDGE], 0.0), lane[:EDGE])

    count = pair_rows()

    def flat(make):
        return jnp.concatenate([make(i, pair_span(i)) for i in range(EDGE)], 1)

    rank = lax.broadcasted_iota(jnp.int32, (total, count), 0)
    one = flat(lambda i, width: jnp.full((1, width), i, jnp.int32))
    other = flat(lambda i, width: lax.broadcasted_iota(jnp.int32, (1, width), 1))
    goal = flat(lambda i, width: target_ref[i : i + 1, :width])
    level = flat(lambda i, width: 2.0 * levels_ref[i : i + 1, :width].astype(jnp.float32))
    level = jnp.where(other <= one, level, 0.0)
    same = other == one
    value = jnp.where(rank == goal, jnp.where(same, 0.5 * level, level), 0.0)
    value = value - jnp.where(rank == one, level, 0.0)
    value = value - jnp.where(rank == other, jnp.where(same, 0.0, level), 0.0)
    square = (total, total)
    row = lax.broadcasted_iota(jnp.int32, square, 0)
    col = lax.broadcasted_iota(jnp.int32, square, 1)
    lower = jnp.where(row <= col, weights_ref[...].astype(jnp.float32), 0.0)
    frag = lower / jnp.sum(lower, axis=0, keepdims=True)
    rate = rate_ref[...]
    linear = (frag * rate - jnp.where(row == col, rate, 0.0)) * (1.0 / half_scale)
    high, low = halves(jnp.concatenate([value, linear], 1))
    pair_ref[:total] = high
    pair_ref[total:] = low


def react(now, quad_ref, pair_ref):
    total = now.shape[0]
    high, low = halves(now)
    stack = jnp.concatenate([high, high, low, low], 0)
    ahead = [now[: pair_span(i)] * now[i : i + 1] for i in range(EDGE)]
    high, low = halves(jnp.concatenate([*ahead, now], 0))

    def dot(table, value):
        return jnp.dot(table, value, preferred_element_type=jnp.float32)

    spans = [(first, STEP * (total - first)) for first in range(EDGE, total, STEP)] + [(None, EDGE)]
    made = {}
    offset = 0
    while spans:
        taken = [spans.pop(0)]
        while spans and sum(count for _, count in taken) + spans[0][1] <= LARGEST:
            taken.append(spans.pop(0))
        count = sum(count for _, count in taken)
        product = dot(quad_ref[offset : offset + count, :], stack)
        offset += count
        start = 0
        for first, count in taken:
            made[first] = product[start : start + count]
            start += count

    gain = None
    for first in range(EDGE, total, STEP):
        count = total - first
        part = made[first][:count] * now[first : first + 1]
        for r in range(1, STEP):
            part = part + made[first][r * count : (r + 1) * count] * now[first + r : first + r + 1]
        skip = first - EDGE
        gain = part if gain is None else jnp.concatenate([gain[:skip], gain[skip:] + part], 0)
    loss = made[None] * now[:EDGE]
    both = dot(pair_ref[...], high)
    rest = both[:total] + both[total:] + dot(pair_ref[:total], low)
    return now + (rest + jnp.concatenate([-loss, gain], 0)) * half_scale


MESH = pl.DeviceIdType.MESH
LAND = 4.0


def step_kernel(
    tiles,
    peers,
    flat_hbm,
    speed_hbm,
    water_hbm,
    settling_hbm,
    rate_hbm,
    levels_hbm,
    target_hbm,
    weights_hbm,
    out_ref,
    speed_ref,
    water_ref,
    settling_ref,
    rate_ref,
    table_ref,
    quad_ref,
    pair_ref,
    field_ref,
    drift_ref,
    halo_ref,
    moved_ref,
    whole_ref,
    done_ref,
    back_ref,
    twin_ref,
    twin_done_ref,
    load_sem,
    drift_recv,
    halo_recv,
    out_send,
    out_recv,
    back_recv,
    twin_sem,
):
    layers, group, columns = moved_ref.shape
    tile_lanes = columns // LANES
    block = CY // LANES * layers
    own = layers // peers
    tile = lax.axis_index("tile")
    me = lax.axis_index("cls")
    has_west = tile > 0
    has_east = tile < tiles - 1

    if peers == 4:
        partners = [lax.rem(me + 2, 4), 3 - me, me + 1 - 2 * lax.rem(me, 2)]
    else:
        partners = [lax.rem(me + d, peers) for d in range(1, peers)]

    twin = lax.rem(me + peers // 2, peers)
    beside = peers - 2

    barrier = pltpu.get_barrier_semaphore()

    @pl.when(has_west)
    def _():
        pl.semaphore_signal(barrier, inc=1, device_id={"tile": tile - 1}, device_id_type=MESH)

    @pl.when(has_east)
    def _():
        pl.semaphore_signal(barrier, inc=1, device_id={"tile": tile + 1}, device_id_type=MESH)

    for p in partners:
        pl.semaphore_signal(barrier, inc=1, device_id={"cls": p}, device_id_type=MESH)

    loads = [
        pltpu.make_async_copy(source, place, load_sem.at[n + 1])
        for n, (source, place) in enumerate(
            (
                (speed_hbm, speed_ref),
                (water_hbm, water_ref),
                (settling_hbm, settling_ref),
                (rate_hbm, rate_ref),
            )
        )
    ]
    for copy in loads[:3]:
        copy.start()
    for x in range(CX):
        for j in range(x * (CY // LANES), (x + 1) * (CY // LANES)):
            for l in range(layers):
                pltpu.make_async_copy(
                    flat_hbm.at[:, j * layers + l, 0, :],
                    field_ref.at[pl.ds(l * group, group), pl.ds(j * LANES, LANES)],
                    load_sem.at[0 if x < CX - 1 else 6],
                ).start()
    for copy in loads[3:]:
        copy.start()
    for n, source in enumerate((levels_hbm, target_hbm, weights_hbm)):
        pltpu.make_async_copy(source, table_ref.at[n], load_sem.at[len(loads) + 1]).start()

    def await_all(ref, sem):
        pltpu.make_async_copy(ref, ref, sem).wait()

    def span(start, width):
        return pl.ds(pl.multiple_of(start, width), width)

    def cols(x):
        return span(x * CY, CY)

    def strip(l):
        return pl.ds(l * group, group)

    for side, exists in ((0, has_west), (1, has_east)):

        @pl.when(jnp.logical_not(exists))
        def _():
            drift_ref[:, cols(side * (CX + 1))] = jnp.full((layers, CY), LAND, jnp.float32)

    for copy in loads[:3]:
        copy.wait()
    drift_ref[:, pl.ds(CY, columns)] = jnp.where(
        jnp.broadcast_to(water_ref[...], (layers, columns)) == 1, speed_ref[0], LAND
    )
    square = (group, group)
    diagonal = lax.broadcasted_iota(jnp.int32, square, 0) == lax.broadcasted_iota(
        jnp.int32, square, 1
    )
    settle = jnp.sum(jnp.where(diagonal, settling_ref[...], 0.0), axis=1, keepdims=True)
    settle = jnp.broadcast_to(settle, (group, CY))

    def enter():
        before = lax.div(tile + tiles - 1, tiles)
        after = lax.div(2 * (tiles - 1) - tile, tiles)
        pl.semaphore_wait(barrier, peers - 1 + before + after)

    far_side = lax.rem(tile, 2)
    sides = (far_side, 1 - far_side)
    edges = [side * (CX - 1) for side in sides]

    def there(way):
        side = sides[way]
        return (1 - side) * tile + side * (tiles - 1 - tile) > 0

    lonely = 1 - lax.div(tile + tiles - 1, tiles) * lax.div(2 * (tiles - 1) - tile, tiles)

    def beyond(way):
        return {"tile": tile - 1 + 2 * sides[way]}

    def drift(way):
        side = sides[way]
        return pltpu.make_async_remote_copy(
            src_ref=drift_ref.at[:, cols(edges[way] + 1)],
            dst_ref=drift_ref.at[:, cols((1 - side) * (CX + 1))],
            send_sem=load_sem.at[way],
            recv_sem=drift_recv.at[way],
            device_id=beyond(way),
            device_id_type=MESH,
        )

    def halo(way, h):
        return pltpu.make_async_remote_copy(
            src_ref=field_ref.at[:, span(edges[way] * CY + h * UNIT, UNIT)],
            dst_ref=halo_ref.at[way, :, pl.ds(h * UNIT, UNIT)],
            send_sem=load_sem.at[2 + way],
            recv_sem=halo_recv.at[way, h],
            device_id=beyond(way),
            device_id_type=MESH,
        )

    def reach_out():
        for way, h in [(way, h) for h in range(SPLIT) for way in range(2)]:

            @pl.when(there(way))
            def _():
                if h == 0:
                    drift(way).start()
                halo(way, h).start()

    def arrival(u):
        inner = (u - SPLIT) // SPLIT + SPLIT
        return u if u < SPLIT else inner if u < (CX - 1) * SPLIT else u - (CX - 2) * (SPLIT - 1)

    def forward(n, u, start, width, s):
        at = span(start, width)
        return pltpu.make_async_remote_copy(
            src_ref=moved_ref.at[partners[n] * own + s, :, at],
            dst_ref=whole_ref.at[s, span(me * group, group), at],
            send_sem=out_send,
            recv_sem=out_recv.at[arrival(u), s],
            device_id={"cls": partners[n]},
            device_id_type=MESH,
        )

    def send(u, start, width):
        for s in range(own):
            for n in range(peers - 1):
                forward(n, u, start, width, s).start()
        at = span(start, width)
        for s in range(own):
            whole_ref[s, span(me * group, group), at] = moved_ref[me * own + s, :, at]

    rows = CX - 2

    def slot(k):
        row = k // SPLIT
        return row + (k % SPLIT if row == CX - 1 else 0)

    def backward(n, k, start, width, s):
        at = span(start, width)
        return pltpu.make_async_remote_copy(
            src_ref=done_ref.at[s, span(partners[n] * group, group), at],
            dst_ref=back_ref.at[me * own + s, :, at],
            send_sem=load_sem.at[5] if k // SPLIT == rows - 1 else load_sem.at[4],
            recv_sem=back_recv.at[slot(k)],
            device_id={"cls": partners[n]},
            device_id_type=MESH,
        )

    def row(at):
        value = drift_ref[:, at]
        return value, jnp.where(value < 0.5 * LAND, 1.0, 0.0)

    def face(one, other):
        return 0.5 * (one[0] + other[0]) * (one[1] * other[1])

    def leaving(flow):
        return jnp.maximum(flow, 0.0)

    def coming(flow):
        return -jnp.minimum(flow, 0.0)

    def transport(x, flows):
        water = row(cols(x + 1))[1]
        v = speed_ref[1, :, cols(x)]
        lane = lax.broadcasted_iota(jnp.int32, v.shape, 1)
        north = 0.5 * (v + pltpu.roll(v, CY - 1, 1)) * (water * pltpu.roll(water, CY - 1, 1))
        north = jnp.where(lane == CY - 1, 0.0, north)
        south = -pltpu.roll(north, 1, 1)
        centre = 1.0 - leaving(north) - leaving(south)
        for flow, _ in flows:
            centre = centre - leaving(flow)
        from_south, from_north = coming(south), coming(north)
        inner = [(coming(flow), at) for flow, at in flows]
        for l in range(layers):
            c = field_ref[strip(l), cols(x)]
            moved = (
                (centre[l : l + 1] - settle) * c
                + from_south[l : l + 1] * pltpu.roll(c, 1, 1)
                + from_north[l : l + 1] * pltpu.roll(c, CY - 1, 1)
            )
            for factor, at in inner:
                moved = moved + factor[l : l + 1] * field_ref[strip(l), cols(at)]
            if l > 0:
                moved = moved + settle * field_ref[strip(l - 1), cols(x)]
            moved_ref[l, :, cols(x)] = moved

    def inner_transport(x):
        here = row(cols(x + 1))
        transport(x, [(-face(row(cols(x)), here), x - 1), (face(here, row(cols(x + 2))), x + 1)])

    def prepare(way):
        x = edges[way]
        inward = 1 - 2 * sides[way]
        flow = face(row(cols(x + 1)), row(cols(x + 1 + inward))) * inward.astype(jnp.float32)
        transport(x, [(flow, x + inward)])

    def close(way, h):
        start = edges[way] * CY + h * UNIT

        @pl.when(there(way))
        def _():
            if h == 0:
                drift(way).wait_recv()
            halo(way, h).wait_recv()
            outward = 2 * sides[way] - 1
            beyond_at = span(sides[way] * (CX + 1) * CY + h * UNIT, UNIT)
            flow = face(row(span(start + CY, UNIT)), row(beyond_at)) * outward.astype(jnp.float32)
            out, back = leaving(flow), coming(flow)
            at = span(start, UNIT)
            for l in range(layers):
                moved_ref[l, :, at] = moved_ref[l, :, at] + (
                    back[l : l + 1] * halo_ref[way, strip(l), pl.ds(h * UNIT, UNIT)]
                    - out[l : l + 1] * field_ref[strip(l), at]
                )

        send((rows + way) * SPLIT + h, start, UNIT)

    double = there(0) if peers == 4 else False
    middle = cols(CX - 2)

    def extra(n, s):
        return pltpu.make_async_remote_copy(
            src_ref=moved_ref.at[lax.rem(partners[n] + peers // 2, peers) * own + s, :, middle],
            dst_ref=twin_ref.at[s, span(me * group, group)],
            send_sem=load_sem.at[6],
            recv_sem=twin_sem,
            device_id={"cls": partners[n]},
            device_id_type=MESH,
        )

    def send_twice():
        for s in range(own):
            for n in range(peers - 1):
                extra(n, s).start()
            twin_ref[s, span(me * group, group)] = moved_ref[twin * own + s, :, middle]

    def twin_back(s):
        return pltpu.make_async_remote_copy(
            src_ref=twin_done_ref.at[s, span(partners[beside] * group, group)],
            dst_ref=back_ref.at[twin * own + s, :, middle],
            send_sem=load_sem.at[5],
            recv_sem=back_recv.at[rows - 1],
            device_id={"cls": partners[beside]},
            device_id_type=MESH,
        )

    def twin_unit():
        await_all(twin_ref.at[:, pl.ds(0, (peers - 1) * group)], twin_sem)
        for s in range(own):
            now = react(twin_ref[s], quad_ref, pair_ref)
            twin_done_ref[s] = react(now, quad_ref, pair_ref)
            twin_back(s).start()
            back_ref[twin * own + s, :, middle] = twin_done_ref[s, span(me * group, group)]

    def send_row(x):
        for h in range(SPLIT):
            send((x - 1) * SPLIT + h, x * CY + h * UNIT, UNIT)

    inner = pl.ds(0, (CX - 1) * CY)
    await_all(field_ref.at[:, inner], load_sem.at[0])
    inner_transport(1)
    await_all(field_ref.at[:, cols(CX - 1)], load_sem.at[6])
    enter()
    reach_out()
    send_row(1)
    for x in range(2, CX - 1):
        inner_transport(x)
        send_row(x)

    @pl.when(double)
    def _():
        send_twice()

    loads[3].wait()
    await_all(table_ref, load_sem.at[len(loads) + 1])
    build_tables(table_ref.at[0], table_ref.at[1], table_ref.at[2], rate_ref, quad_ref, pair_ref)

    prepare(0)
    prepare(1)

    @pl.when(jnp.logical_not(there(0)))
    def _():
        for h in range(SPLIT):
            close(0, h)

    def unit(u, start, width):
        at = span(start, width)
        for s in range(own):
            await_all(whole_ref.at[s, pl.ds(0, (peers - 1) * group), at], out_recv.at[arrival(u), s])
            now = react(whole_ref[s, :, at], quad_ref, pair_ref)
            done_ref[s, :, at] = react(now, quad_ref, pair_ref)
            back_ref[me * own + s, :, at] = done_ref[s, span(me * group, group), at]

    def start_of(k):
        q, h = divmod(k, SPLIT)
        return (q + 1 if q < rows else edges[q - rows]) * CY + h * UNIT

    def give_back(k):
        for s in range(own):
            for n in range(peers - 1):
                backward(n, k, start_of(k), UNIT, s).start()

    def act(name):
        kind, *rest = name
        if kind == "unit":
            k, wide = rest
            unit(k, start_of(k), CY if wide else UNIT)
        elif kind == "back":
            if rest[0] // SPLIT == rows - 1:
                pl.when(jnp.logical_not(double))(lambda: give_back(rest[0]))
            else:
                give_back(rest[0])
        elif kind == "beside":
            @pl.when(double)
            def _():
                for s in range(own):
                    for h in range(SPLIT):
                        k = (rows - 1) * SPLIT + h
                        backward(beside, k, start_of(k), UNIT, s).start()
        elif kind == "twin":
            pl.when(double)(twin_unit)
        elif kind == "far":
            @pl.when(there(0))
            def _():
                close(0, rest[0])
        else:
            @pl.when(lonely == (1 if kind == "alone" else 0))
            def _():
                close(1, rest[0])

    for name in PLAN:
        act(name)

    for way in range(2):

        @pl.when(there(way))
        def _():
            drift(way).wait_send()
            await_all(halo_ref.at[way], load_sem.at[2 + way])

    def settle_out(start, width):
        for l in range(layers):
            for j in range(width // LANES):
                at = (lax.div(start, LANES) + j) * layers + l
                out_ref[pl.ds(at, group, stride=tile_lanes * layers), :] = back_ref[
                    l, :, span(start + j * LANES, LANES)
                ]

    def finish(u, start, width):
        await_all(
            back_ref.at[pl.ds(0, (peers - 1) * own), :, span(start, width)], back_recv.at[u]
        )
        settle_out(start, width)

    await_all(moved_ref.at[pl.ds(0, (peers - 1) * own)], out_send)
    for q in range(rows - 1):
        finish(q, (q + 1) * CY, CY)

    @pl.when(double)
    def _():
        await_all(twin_ref.at[:, pl.ds(0, (peers - 1) * group)], load_sem.at[6])
        await_all(twin_ref.at[:, pl.ds(0, 2 * group)], load_sem.at[5])
        await_all(back_ref.at[pl.ds(0, 2 * own), :, middle], back_recv.at[rows - 1])

    @pl.when(jnp.logical_not(double))
    def _():
        await_all(done_ref.at[:, pl.ds(0, (peers - 1) * group), middle], load_sem.at[5])
        await_all(back_ref.at[pl.ds(0, (peers - 1) * own), :, middle], back_recv.at[rows - 1])

    settle_out((CX - 2) * CY, CY)
    finish(rows, edges[0] * CY, CY)
    for h in range(SPLIT):
        finish(rows + 1 + h, edges[1] * CY + h * UNIT, UNIT)
    await_all(done_ref.at[:, pl.ds(0, (peers - 1) * group), pl.ds(0, (CX - 1) * CY)], load_sem.at[4])


PLAN = (
    ("unit", 0, 0),
    ("back", 0),
    ("far", 0),
    ("unit", 1, 0),
    ("far", 1),
    ("back", 1),
    ("alone", 0),
    ("alone", 1),
    ("unit", 2, 1),
    ("beside",),
    ("back", 2),
    ("back", 3),
    ("near", 0),
    ("twin",),
    ("near", 1),
    ("unit", 4, 1),
    ("back", 4),
    ("back", 5),
    ("unit", 6, 0),
    ("back", 6),
    ("unit", 7, 0),
    ("back", 7),
)


def body(
    tiles,
    peers,
    concentration,
    velocity,
    land_mask,
    settling,
    breakage_rate,
    kernel_levels,
    pair_target,
    fragment_weights,
):
    group, layers, columns = concentration.shape
    total = kernel_levels.shape[0]
    own = layers // peers
    flat = concentration.reshape(group, layers, columns // LANES, LANES)
    flat = jnp.transpose(flat, (0, 2, 1, 3)).reshape(group, -1, 1, LANES)
    operands = (
        flat,
        velocity,
        land_mask.reshape(1, columns),
        settling.reshape(1, group),
        breakage_rate.reshape(1, total),
        kernel_levels,
        pair_target,
        fragment_weights,
    )
    dma = pltpu.SemaphoreType.DMA
    done = pl.pallas_call(
        functools.partial(step_kernel, tiles, peers),
        out_shape=pltpu.VMEM((group * layers * columns // LANES, LANES), jnp.float32),
        in_specs=[pl.BlockSpec(memory_space=pl.ANY)] * len(operands),
        out_specs=pl.BlockSpec(memory_space=pltpu.VMEM),
        scratch_shapes=[
            *[pltpu.VMEM(x.shape, x.dtype) for x in operands[1:5]],
            pltpu.VMEM((3, total, total), jnp.int32),
            pltpu.VMEM((quad_rows(total), 4 * total), jnp.bfloat16),
            pltpu.VMEM((2 * total, pair_rows() + total), jnp.bfloat16),
            pltpu.VMEM((layers * group, columns), jnp.float32),
            pltpu.VMEM((layers, columns + 2 * CY), jnp.float32),
            pltpu.VMEM((2, layers * group, CY), jnp.float32),
            pltpu.VMEM((layers, group, columns), jnp.float32),
            pltpu.VMEM((own, total, columns), jnp.float32),
            pltpu.VMEM((own, total, columns), jnp.float32),
            pltpu.VMEM((layers, group, columns), jnp.float32),
            pltpu.VMEM((own, total, CY), jnp.float32),
            pltpu.VMEM((own, total, CY), jnp.float32),
            dma((7,)),
            dma((2,)),
            dma((2, SPLIT)),
            dma,
            dma((UNITS, own)),
            dma((CX - 1 + SPLIT,)),
            dma,
        ],
        compiler_params=pltpu.CompilerParams(collective_id=0, has_side_effects=True),
    )(*operands)
    done = done.reshape(group, columns // LANES, layers, LANES)
    return jnp.transpose(done, (0, 2, 1, 3)).reshape(group, layers, columns)


def solution(mesh):
    return jax.shard_map(
        functools.partial(body, mesh.shape["tile"], mesh.shape["cls"]),
        mesh=mesh,
        in_specs=(
            P("cls", None, "tile"),
            P(None, None, "tile"),
            P("tile"),
            P("cls"),
            P(),
            P(),
            P(),
            P(),
        ),
        out_specs=P("cls", None, "tile"),
        check_vma=False,
    )
```

```python
import functools

import jax
import jax.numpy as jnp
from jax import lax
from jax.experimental import pallas as pl
from jax.experimental.pallas import tpu as pltpu
from jax.sharding import PartitionSpec as P

CY = 512
CX = 4
half_scale = 0.5e-05
STEP = 8
EDGE = 24
LARGEST = 448
LANES = 128
SPLIT = 2
UNIT = CY // SPLIT
UNITS = CX - 2 + 2 * SPLIT


def split_pair(value, lane, total):
    high = value.astype(jnp.bfloat16).astype(jnp.float32)
    return jnp.where(lane < total, high, value - high).astype(jnp.bfloat16)


def halves(value):
    high = value.astype(jnp.bfloat16)
    return high, (value - high.astype(jnp.float32)).astype(jnp.bfloat16)


def pair_span(i):
    return STEP * (i // STEP + 1)


def quad_rows(total):
    return sum(STEP * (total - first) for first in range(EDGE, total, STEP)) + EDGE


def pair_rows():
    return sum(pair_span(i) for i in range(EDGE))


def build_tables(levels_ref, target_ref, weights_ref, rate_ref, quad_ref, pair_ref):
    total = levels_ref.shape[0]
    wide = 2 * total
    narrow = levels_ref[...].astype(jnp.float32)
    levels = jnp.concatenate([narrow, narrow], 1)
    target = target_ref[...]
    target = jnp.concatenate([target, target], 1)
    row = lax.broadcasted_iota(jnp.int32, (total, wide), 0)
    lane = lax.broadcasted_iota(jnp.int32, (total, wide), 1)
    col = jnp.where(lane < total, lane, lane - total)
    twice = 2.0 * levels
    birth = jnp.where(col < row, twice, jnp.where(col == row, levels, 0.0))

    def put(offset, value, lane):
        count = value.shape[0]
        packed = split_pair(value, lane, total)
        quad_ref[offset : offset + count, :wide] = packed
        quad_ref[offset : offset + count, wide:] = packed
        return offset + count

    offset = 0
    for first in range(EDGE, total, STEP):
        rank = row[first:]
        for i in range(first, first + STEP):
            value = jnp.where(target[i : i + 1] == rank, birth[i : i + 1], 0.0)
            value = value - jnp.where(rank == i, twice[i : i + 1], 0.0)
            offset = put(offset, value, lane[first:])
    put(offset, jnp.where(col[:EDGE] >= EDGE, twice[:EDGE], 0.0), lane[:EDGE])

    count = pair_rows()

    def flat(make):
        return jnp.concatenate([make(i, pair_span(i)) for i in range(EDGE)], 1)

    rank = lax.broadcasted_iota(jnp.int32, (total, count), 0)
    one = flat(lambda i, width: jnp.full((1, width), i, jnp.int32))
    other = flat(lambda i, width: lax.broadcasted_iota(jnp.int32, (1, width), 1))
    goal = flat(lambda i, width: target_ref[i : i + 1, :width])
    level = flat(lambda i, width: 2.0 * levels_ref[i : i + 1, :width].astype(jnp.float32))
    level = jnp.where(other <= one, level, 0.0)
    same = other == one
    value = jnp.where(rank == goal, jnp.where(same, 0.5 * level, level), 0.0)
    value = value - jnp.where(rank == one, level, 0.0)
    value = value - jnp.where(rank == other, jnp.where(same, 0.0, level), 0.0)
    square = (total, total)
    row = lax.broadcasted_iota(jnp.int32, square, 0)
    col = lax.broadcasted_iota(jnp.int32, square, 1)
    lower = jnp.where(row <= col, weights_ref[...].astype(jnp.float32), 0.0)
    frag = lower / jnp.sum(lower, axis=0, keepdims=True)
    rate = rate_ref[...]
    linear = (frag * rate - jnp.where(row == col, rate, 0.0)) * (1.0 / half_scale)
    high, low = halves(jnp.concatenate([value, linear], 1))
    pair_ref[:total] = high
    pair_ref[total:] = low


def react(now, quad_ref, pair_ref):
    total = now.shape[0]
    high, low = halves(now)
    stack = jnp.concatenate([high, high, low, low], 0)
    ahead = [now[: pair_span(i)] * now[i : i + 1] for i in range(EDGE)]
    high, low = halves(jnp.concatenate([*ahead, now], 0))

    def dot(table, value):
        return jnp.dot(table, value, preferred_element_type=jnp.float32)

    spans = [(first, STEP * (total - first)) for first in range(EDGE, total, STEP)] + [(None, EDGE)]
    made = {}
    offset = 0
    while spans:
        taken = [spans.pop(0)]
        while spans and sum(count for _, count in taken) + spans[0][1] <= LARGEST:
            taken.append(spans.pop(0))
        count = sum(count for _, count in taken)
        product = dot(quad_ref[offset : offset + count, :], stack)
        offset += count
        start = 0
        for first, count in taken:
            made[first] = product[start : start + count]
            start += count

    gain = None
    for first in range(EDGE, total, STEP):
        count = total - first
        part = made[first][:count] * now[first : first + 1]
        for r in range(1, STEP):
            part = part + made[first][r * count : (r + 1) * count] * now[first + r : first + r + 1]
        skip = first - EDGE
        gain = part if gain is None else jnp.concatenate([gain[:skip], gain[skip:] + part], 0)
    loss = made[None] * now[:EDGE]
    both = dot(pair_ref[...], high)
    rest = both[:total] + both[total:] + dot(pair_ref[:total], low)
    return now + (rest + jnp.concatenate([-loss, gain], 0)) * half_scale


MESH = pl.DeviceIdType.MESH
LAND = 4.0


def step_kernel(
    tiles,
    peers,
    flat_hbm,
    speed_hbm,
    water_hbm,
    settling_hbm,
    rate_hbm,
    levels_hbm,
    target_hbm,
    weights_hbm,
    out_ref,
    speed_ref,
    water_ref,
    settling_ref,
    rate_ref,
    table_ref,
    quad_ref,
    pair_ref,
    field_ref,
    drift_ref,
    halo_ref,
    moved_ref,
    whole_ref,
    done_ref,
    back_ref,
    twin_ref,
    twin_done_ref,
    load_sem,
    drift_recv,
    halo_recv,
    out_send,
    out_recv,
    back_recv,
    twin_sem,
):
    layers, group, columns = moved_ref.shape
    tile_lanes = columns // LANES
    block = CY // LANES * layers
    own = layers // peers
    tile = lax.axis_index("tile")
    me = lax.axis_index("cls")
    has_west = tile > 0
    has_east = tile < tiles - 1

    if peers == 4:
        partners = [lax.rem(me + 2, 4), 3 - me, me + 1 - 2 * lax.rem(me, 2)]
    else:
        partners = [lax.rem(me + d, peers) for d in range(1, peers)]

    twin = lax.rem(me + peers // 2, peers)
    beside = peers - 2

    barrier = pltpu.get_barrier_semaphore()

    @pl.when(has_west)
    def _():
        pl.semaphore_signal(barrier, inc=1, device_id={"tile": tile - 1}, device_id_type=MESH)

    @pl.when(has_east)
    def _():
        pl.semaphore_signal(barrier, inc=1, device_id={"tile": tile + 1}, device_id_type=MESH)

    for p in partners:
        pl.semaphore_signal(barrier, inc=1, device_id={"cls": p}, device_id_type=MESH)

    loads = [
        pltpu.make_async_copy(source, place, load_sem.at[n + 1])
        for n, (source, place) in enumerate(
            (
                (speed_hbm, speed_ref),
                (water_hbm, water_ref),
                (settling_hbm, settling_ref),
                (rate_hbm, rate_ref),
            )
        )
    ]
    for copy in loads[:3]:
        copy.start()
    for x in range(CX):
        for j in range(x * (CY // LANES), (x + 1) * (CY // LANES)):
            for l in range(layers):
                pltpu.make_async_copy(
                    flat_hbm.at[:, j * layers + l, 0, :],
                    field_ref.at[pl.ds(l * group, group), pl.ds(j * LANES, LANES)],
                    load_sem.at[0 if x < CX - 1 else 6],
                ).start()
    for copy in loads[3:]:
        copy.start()
    for n, source in enumerate((levels_hbm, target_hbm, weights_hbm)):
        pltpu.make_async_copy(source, table_ref.at[n], load_sem.at[len(loads) + 1]).start()

    def await_all(ref, sem):
        pltpu.make_async_copy(ref, ref, sem).wait()

    def span(start, width):
        return pl.ds(pl.multiple_of(start, width), width)

    def cols(x):
        return span(x * CY, CY)

    def strip(l):
        return pl.ds(l * group, group)

    for side, exists in ((0, has_west), (1, has_east)):

        @pl.when(jnp.logical_not(exists))
        def _():
            drift_ref[:, cols(side * (CX + 1))] = jnp.full((layers, CY), LAND, jnp.float32)

    for copy in loads[:3]:
        copy.wait()
    drift_ref[:, pl.ds(CY, columns)] = jnp.where(
        jnp.broadcast_to(water_ref[...], (layers, columns)) == 1, speed_ref[0], LAND
    )
    square = (group, group)
    diagonal = lax.broadcasted_iota(jnp.int32, square, 0) == lax.broadcasted_iota(
        jnp.int32, square, 1
    )
    settle = jnp.sum(jnp.where(diagonal, settling_ref[...], 0.0), axis=1, keepdims=True)
    settle = jnp.broadcast_to(settle, (group, CY))

    def enter():
        before = lax.div(tile + tiles - 1, tiles)
        after = lax.div(2 * (tiles - 1) - tile, tiles)
        pl.semaphore_wait(barrier, peers - 1 + before + after)

    far_side = lax.rem(tile, 2)
    sides = (far_side, 1 - far_side)
    edges = [side * (CX - 1) for side in sides]

    def there(way):
        side = sides[way]
        return (1 - side) * tile + side * (tiles - 1 - tile) > 0

    lonely = 1 - lax.div(tile + tiles - 1, tiles) * lax.div(2 * (tiles - 1) - tile, tiles)

    def beyond(way):
        return {"tile": tile - 1 + 2 * sides[way]}

    def drift(way):
        side = sides[way]
        return pltpu.make_async_remote_copy(
            src_ref=drift_ref.at[:, cols(edges[way] + 1)],
            dst_ref=drift_ref.at[:, cols((1 - side) * (CX + 1))],
            send_sem=load_sem.at[way],
            recv_sem=drift_recv.at[way],
            device_id=beyond(way),
            device_id_type=MESH,
        )

    def halo(way, h):
        return pltpu.make_async_remote_copy(
            src_ref=field_ref.at[:, span(edges[way] * CY + h * UNIT, UNIT)],
            dst_ref=halo_ref.at[way, :, pl.ds(h * UNIT, UNIT)],
            send_sem=load_sem.at[2 + way],
            recv_sem=halo_recv.at[way, h],
            device_id=beyond(way),
            device_id_type=MESH,
        )

    def reach_out():
        for way, h in [(way, h) for h in range(SPLIT) for way in range(2)]:

            @pl.when(there(way))
            def _():
                if h == 0:
                    drift(way).start()
                halo(way, h).start()

    def arrival(u):
        inner = (u - SPLIT) // SPLIT + SPLIT
        return u if u < SPLIT else inner if u < (CX - 1) * SPLIT else u - (CX - 2) * (SPLIT - 1)

    def forward(n, u, start, width, s):
        at = span(start, width)
        return pltpu.make_async_remote_copy(
            src_ref=moved_ref.at[partners[n] * own + s, :, at],
            dst_ref=whole_ref.at[s, span(me * group, group), at],
            send_sem=out_send,
            recv_sem=out_recv.at[arrival(u), s],
            device_id={"cls": partners[n]},
            device_id_type=MESH,
        )

    def send(u, start, width):
        for s in range(own):
            for n in range(peers - 1):
                forward(n, u, start, width, s).start()
        at = span(start, width)
        for s in range(own):
            whole_ref[s, span(me * group, group), at] = moved_ref[me * own + s, :, at]

    rows = CX - 2

    def slot(k):
        row = k // SPLIT
        return row + (k % SPLIT if row == CX - 1 else 0)

    def backward(n, k, start, width, s):
        at = span(start, width)
        return pltpu.make_async_remote_copy(
            src_ref=done_ref.at[s, span(partners[n] * group, group), at],
            dst_ref=back_ref.at[me * own + s, :, at],
            send_sem=load_sem.at[5] if k // SPLIT == rows - 1 else load_sem.at[4],
            recv_sem=back_recv.at[slot(k)],
            device_id={"cls": partners[n]},
            device_id_type=MESH,
        )

    def row(at):
        value = drift_ref[:, at]
        return value, jnp.where(value < 0.5 * LAND, 1.0, 0.0)

    def face(one, other):
        return 0.5 * (one[0] + other[0]) * (one[1] * other[1])

    def leaving(flow):
        return jnp.maximum(flow, 0.0)

    def coming(flow):
        return -jnp.minimum(flow, 0.0)

    def transport(x, flows):
        water = row(cols(x + 1))[1]
        v = speed_ref[1, :, cols(x)]
        lane = lax.broadcasted_iota(jnp.int32, v.shape, 1)
        north = 0.5 * (v + pltpu.roll(v, CY - 1, 1)) * (water * pltpu.roll(water, CY - 1, 1))
        north = jnp.where(lane == CY - 1, 0.0, north)
        south = -pltpu.roll(north, 1, 1)
        centre = 1.0 - leaving(north) - leaving(south)
        for flow, _ in flows:
            centre = centre - leaving(flow)
        from_south, from_north = coming(south), coming(north)
        inner = [(coming(flow), at) for flow, at in flows]
        for l in range(layers):
            c = field_ref[strip(l), cols(x)]
            moved = (
                (centre[l : l + 1] - settle) * c
                + from_south[l : l + 1] * pltpu.roll(c, 1, 1)
                + from_north[l : l + 1] * pltpu.roll(c, CY - 1, 1)
            )
            for factor, at in inner:
                moved = moved + factor[l : l + 1] * field_ref[strip(l), cols(at)]
            if l > 0:
                moved = moved + settle * field_ref[strip(l - 1), cols(x)]
            moved_ref[l, :, cols(x)] = moved

    def inner_transport(x):
        here = row(cols(x + 1))
        transport(x, [(-face(row(cols(x)), here), x - 1), (face(here, row(cols(x + 2))), x + 1)])

    def prepare(way):
        x = edges[way]
        inward = 1 - 2 * sides[way]
        flow = face(row(cols(x + 1)), row(cols(x + 1 + inward))) * inward.astype(jnp.float32)
        transport(x, [(flow, x + inward)])

    def close(way, h):
        start = edges[way] * CY + h * UNIT

        @pl.when(there(way))
        def _():
            if h == 0:
                drift(way).wait_recv()
            halo(way, h).wait_recv()
            outward = 2 * sides[way] - 1
            beyond_at = span(sides[way] * (CX + 1) * CY + h * UNIT, UNIT)
            flow = face(row(span(start + CY, UNIT)), row(beyond_at)) * outward.astype(jnp.float32)
            out, back = leaving(flow), coming(flow)
            at = span(start, UNIT)
            for l in range(layers):
                moved_ref[l, :, at] = moved_ref[l, :, at] + (
                    back[l : l + 1] * halo_ref[way, strip(l), pl.ds(h * UNIT, UNIT)]
                    - out[l : l + 1] * field_ref[strip(l), at]
                )

        send((rows + way) * SPLIT + h, start, UNIT)

    double = there(0) if peers == 4 else False
    middle = cols(CX - 2)

    def extra(n, s):
        return pltpu.make_async_remote_copy(
            src_ref=moved_ref.at[lax.rem(partners[n] + peers // 2, peers) * own + s, :, middle],
            dst_ref=twin_ref.at[s, span(me * group, group)],
            send_sem=load_sem.at[6],
            recv_sem=twin_sem,
            device_id={"cls": partners[n]},
            device_id_type=MESH,
        )

    def send_twice():
        for s in range(own):
            for n in range(peers - 1):
                extra(n, s).start()
            twin_ref[s, span(me * group, group)] = moved_ref[twin * own + s, :, middle]

    def twin_back(s):
        return pltpu.make_async_remote_copy(
            src_ref=twin_done_ref.at[s, span(partners[beside] * group, group)],
            dst_ref=back_ref.at[twin * own + s, :, middle],
            send_sem=load_sem.at[5],
            recv_sem=back_recv.at[rows - 1],
            device_id={"cls": partners[beside]},
            device_id_type=MESH,
        )

    def twin_unit():
        await_all(twin_ref.at[:, pl.ds(0, (peers - 1) * group)], twin_sem)
        for s in range(own):
            now = react(twin_ref[s], quad_ref, pair_ref)
            twin_done_ref[s] = react(now, quad_ref, pair_ref)
            twin_back(s).start()
            back_ref[twin * own + s, :, middle] = twin_done_ref[s, span(me * group, group)]

    def send_row(x):
        for h in range(SPLIT):
            send((x - 1) * SPLIT + h, x * CY + h * UNIT, UNIT)

    inner = pl.ds(0, (CX - 1) * CY)
    await_all(field_ref.at[:, inner], load_sem.at[0])
    inner_transport(1)
    await_all(field_ref.at[:, cols(CX - 1)], load_sem.at[6])
    enter()
    reach_out()
    send_row(1)
    for x in range(2, CX - 1):
        inner_transport(x)
        send_row(x)

    @pl.when(double)
    def _():
        send_twice()

    loads[3].wait()
    await_all(table_ref, load_sem.at[len(loads) + 1])
    build_tables(table_ref.at[0], table_ref.at[1], table_ref.at[2], rate_ref, quad_ref, pair_ref)

    prepare(0)
    prepare(1)

    @pl.when(jnp.logical_not(there(0)))
    def _():
        for h in range(SPLIT):
            close(0, h)

    def unit(u, start, width):
        at = span(start, width)
        for s in range(own):
            await_all(whole_ref.at[s, pl.ds(0, (peers - 1) * group), at], out_recv.at[arrival(u), s])
            now = react(whole_ref[s, :, at], quad_ref, pair_ref)
            done_ref[s, :, at] = react(now, quad_ref, pair_ref)
            back_ref[me * own + s, :, at] = done_ref[s, span(me * group, group), at]

    def start_of(k):
        q, h = divmod(k, SPLIT)
        return (q + 1 if q < rows else edges[q - rows]) * CY + h * UNIT

    def give_back(k):
        for s in range(own):
            for n in range(peers - 1):
                backward(n, k, start_of(k), UNIT, s).start()

    def act(name):
        kind, *rest = name
        if kind == "unit":
            k, wide = rest
            unit(k, start_of(k), CY if wide else UNIT)
        elif kind == "back":
            if rest[0] // SPLIT == rows - 1:
                pl.when(jnp.logical_not(double))(lambda: give_back(rest[0]))
            else:
                give_back(rest[0])
        elif kind == "beside":
            @pl.when(double)
            def _():
                for s in range(own):
                    for h in range(SPLIT):
                        k = (rows - 1) * SPLIT + h
                        backward(beside, k, start_of(k), UNIT, s).start()
        elif kind == "twin":
            pl.when(double)(twin_unit)
        elif kind == "far":
            @pl.when(there(0))
            def _():
                close(0, rest[0])
        else:
            @pl.when(lonely == (1 if kind == "alone" else 0))
            def _():
                close(1, rest[0])

    for name in PLAN:
        act(name)

    for way in range(2):

        @pl.when(there(way))
        def _():
            drift(way).wait_send()
            await_all(halo_ref.at[way], load_sem.at[2 + way])

    def settle_out(start, width):
        for l in range(layers):
            for j in range(width // LANES):
                at = (lax.div(start, LANES) + j) * layers + l
                out_ref[pl.ds(at, group, stride=tile_lanes * layers), :] = back_ref[
                    l, :, span(start + j * LANES, LANES)
                ]

    def finish(u, start, width):
        await_all(
            back_ref.at[pl.ds(0, (peers - 1) * own), :, span(start, width)], back_recv.at[u]
        )
        settle_out(start, width)

    await_all(moved_ref.at[pl.ds(0, (peers - 1) * own)], out_send)
    for q in range(rows - 1):
        finish(q, (q + 1) * CY, CY)

    @pl.when(double)
    def _():
        await_all(twin_ref.at[:, pl.ds(0, (peers - 1) * group)], load_sem.at[6])
        await_all(twin_ref.at[:, pl.ds(0, 2 * group)], load_sem.at[5])
        await_all(back_ref.at[pl.ds(0, 2 * own), :, middle], back_recv.at[rows - 1])

    @pl.when(jnp.logical_not(double))
    def _():
        await_all(done_ref.at[:, pl.ds(0, (peers - 1) * group), middle], load_sem.at[5])
        await_all(back_ref.at[pl.ds(0, (peers - 1) * own), :, middle], back_recv.at[rows - 1])

    settle_out((CX - 2) * CY, CY)
    finish(rows, edges[0] * CY, CY)
    for h in range(SPLIT):
        finish(rows + 1 + h, edges[1] * CY + h * UNIT, UNIT)
    await_all(done_ref.at[:, pl.ds(0, (peers - 1) * group), pl.ds(0, (CX - 1) * CY)], load_sem.at[4])


PLAN = (
    ("unit", 0, 0),
    ("back", 0),
    ("far", 0),
    ("unit", 1, 0),
    ("far", 1),
    ("back", 1),
    ("alone", 0),
    ("alone", 1),
    ("unit", 2, 1),
    ("beside",),
    ("back", 2),
    ("back", 3),
    ("near", 0),
    ("twin",),
    ("near", 1),
    ("unit", 4, 1),
    ("back", 4),
    ("back", 5),
    ("unit", 6, 0),
    ("back", 6),
    ("unit", 7, 0),
    ("back", 7),
)


def body(
    tiles,
    peers,
    concentration,
    velocity,
    land_mask,
    settling,
    breakage_rate,
    kernel_levels,
    pair_target,
    fragment_weights,
):
    group, layers, columns = concentration.shape
    total = kernel_levels.shape[0]
    own = layers // peers
    flat = concentration.reshape(group, layers, columns // LANES, LANES)
    flat = jnp.transpose(flat, (0, 2, 1, 3)).reshape(group, -1, 1, LANES)
    operands = (
        flat,
        velocity,
        land_mask.reshape(1, columns),
        settling.reshape(1, group),
        breakage_rate.reshape(1, total),
        kernel_levels,
        pair_target,
        fragment_weights,
    )
    dma = pltpu.SemaphoreType.DMA
    done = pl.pallas_call(
        functools.partial(step_kernel, tiles, peers),
        out_shape=pltpu.VMEM((group * layers * columns // LANES, LANES), jnp.float32),
        in_specs=[pl.BlockSpec(memory_space=pl.ANY)] * len(operands),
        out_specs=pl.BlockSpec(memory_space=pltpu.VMEM),
        scratch_shapes=[
            *[pltpu.VMEM(x.shape, x.dtype) for x in operands[1:5]],
            pltpu.VMEM((3, total, total), jnp.int32),
            pltpu.VMEM((quad_rows(total), 4 * total), jnp.bfloat16),
            pltpu.VMEM((2 * total, pair_rows() + total), jnp.bfloat16),
            pltpu.VMEM((layers * group, columns), jnp.float32),
            pltpu.VMEM((layers, columns + 2 * CY), jnp.float32),
            pltpu.VMEM((2, layers * group, CY), jnp.float32),
            pltpu.VMEM((layers, group, columns), jnp.float32),
            pltpu.VMEM((own, total, columns), jnp.float32),
            pltpu.VMEM((own, total, columns), jnp.float32),
            pltpu.VMEM((layers, group, columns), jnp.float32),
            pltpu.VMEM((own, total, CY), jnp.float32),
            pltpu.VMEM((own, total, CY), jnp.float32),
            dma((7,)),
            dma((2,)),
            dma((2, SPLIT)),
            dma,
            dma((UNITS, own)),
            dma((CX - 1 + SPLIT,)),
            dma,
        ],
        compiler_params=pltpu.CompilerParams(collective_id=0, has_side_effects=True),
    )(*operands)
    done = done.reshape(group, columns // LANES, layers, LANES)
    return jnp.transpose(done, (0, 2, 1, 3)).reshape(group, layers, columns)


def solution(mesh):
    return jax.shard_map(
        functools.partial(body, mesh.shape["tile"], mesh.shape["cls"]),
        mesh=mesh,
        in_specs=(
            P("cls", None, "tile"),
            P(None, None, "tile"),
            P("tile"),
            P("cls"),
            P(),
            P(),
            P(),
            P(),
        ),
        out_specs=P("cls", None, "tile"),
        check_vma=False,
    )
```
